512 devices in a mesh: cell: 8 (over x, core), own: 64 (over y, z).
Axes of the slice: x: 4, y: 8, z: 8, core: 2. Of those that a mesh axis runs over, the one named last changes fastest.
Arguments:
- gaussians: float32 [4096, 9, 128], P(('cell', 'own')), may hold values from -10 to 16, as said below
- fetch_ids: int32 [8, 64, 64, 4], P('cell', 'own'), may hold values from 0 to 511, as said below
- tile_lists: int32 [8, 64, 12], P('cell', 'own'), may hold values from 0 to 255, as said below
- counts: int32 [8, 64], P('cell', 'own'), may hold values from 6 to 12
- cell_rank: int32 [64, 8], P('own'), may hold values from 0 to 7, each once within a row
- d_colour: float32 [64, 3, 256], P('own', None, 'cell'), may hold values from -96 to 96
Outputs:
- colour: float32 [64, 3, 256], P('own', None, 'cell')
- grads: float32 [4096, 9, 128], P(('cell', 'own'))
The draws below stay inside these ranges and needn't reach their ends.
Inputs may be any that keep to these rules, and one draw needn't show every extreme that they name: `gaussians`: rows of a block along the second dimension: mean x and y in the tile's pixel frame (0 to 16), la and lc (-3 to 0.3), rho (-0.7 to 0.7), logit (-10 to -6), red, green, blue (0 to 1). fetch_ids[c, o, p, :] are 4 different numbers from p * 8 to (p + 1) * 8 - 1. `tile_lists`: each list holds 12 different slots.
All inputs are finite; a program needn't handle non-finite values.
Results may differ from the reference program's by a relative error of at most 0.0003.
Values sent between devices are 32-bit elements; how exact they have to be, the bound alone decides.
A program may use at most 64 MiB of HBM per device.

```python
import jax
import jax.numpy as jnp
from jax import lax

TILE_SIDE = 16
PIX = 256
GP = 128
LIST = 12
CAP = 4
BLK_DEV = 8
TILE_DEV = 1
TILES = 64
N_CELL = 8
N_OWN = 64


def draw_gaussians(key, part):
    subkeys = jax.random.split(key, 9)
    array_shape = (BLK_DEV * N_CELL * N_OWN, GP)
    mean_x = jax.random.uniform(subkeys[0], array_shape, jnp.float32, 0.0, TILE_SIDE)
    mean_y = jax.random.uniform(subkeys[1], array_shape, jnp.float32, 0.0, TILE_SIDE)
    log_a = jax.random.uniform(subkeys[2], array_shape, jnp.float32, -2.8, 0.0)
    log_c = jax.random.uniform(subkeys[3], array_shape, jnp.float32, -2.8, 0.0)
    corr = jax.random.uniform(subkeys[4], array_shape, jnp.float32, -0.7, 0.7)
    logit = jax.random.uniform(subkeys[5], array_shape, jnp.float32, -10.0, -6.0)
    reds = jax.random.uniform(subkeys[6], array_shape, jnp.float32)
    greens = jax.random.uniform(subkeys[7], array_shape, jnp.float32)
    blues = jax.random.uniform(subkeys[8], array_shape, jnp.float32)
    return jnp.stack([mean_x, mean_y, log_a, log_c, corr, logit, reds, greens, blues], axis=1).astype(jnp.float32)


def draw_fetch_ids(key, part):
    scores = jax.random.randint(key, (N_CELL, N_OWN, N_OWN, BLK_DEV), 0, 1 << 20) * BLK_DEV
    scores = scores + jnp.arange(BLK_DEV, dtype=jnp.int32)
    ranked = jnp.argsort(scores, axis=-1, stable=True).astype(jnp.int32)[..., :CAP]
    offsets = (jnp.arange(N_OWN, dtype=jnp.int32) * BLK_DEV)[None, None, :, None]
    return (ranked + offsets).astype(jnp.int32)


def draw_tile_lists(key, part):
    slot_total = N_OWN * CAP
    scores = jax.random.randint(key, (N_CELL, TILE_DEV * N_OWN, slot_total), 0, 1 << 20) * slot_total
    scores = scores + jnp.arange(slot_total, dtype=jnp.int32)
    ranked = jnp.argsort(scores, axis=-1, stable=True).astype(jnp.int32)
    return ranked[..., :LIST].astype(jnp.int32)


def place_ends(entries, own_key, least, largest):
    shape = entries.shape
    place = [jax.random.randint(jax.random.fold_in(own_key, axis), (), 0, shape[axis]) for axis in range(len(shape))]
    entries = entries.at[tuple(place)].set(least)
    longest = shape.index(max(shape))
    place[longest] = (place[longest] + 1) % shape[longest]
    return entries.at[tuple(place)].set(largest)


def shard_levels(stream_key, extent, shards, smallest, high):
    level = 1.0
    for position, shards_of in shards:
        draws = jax.random.uniform(jax.random.fold_in(jax.random.fold_in(stream_key, 6), position), (shards_of,), jnp.float32, smallest / len(shards), high / len(shards))
        level = level * jnp.repeat(jnp.exp(draws), extent[position] // shards_of).reshape((-1,) + (1,) * (len(extent) - 1 - position))
    return level


def centred(rng, dims, spread, most, cuts=(), held_as=jnp.bfloat16):
    result = spread * jax.random.normal(rng, dims, jnp.float32)
    if cuts:
        result = result * shard_levels(rng, dims, cuts, -0.22, 0.18)
    return jnp.clip(result, -most, most).astype(held_as)


def setup_inputs(seed: int = 0) -> dict:
    streams_of = jax.random.split(jax.random.key(seed), 7)
    gaussians = draw_gaussians(jax.random.fold_in(streams_of[6], 71), 0)
    fetch_ids = draw_fetch_ids(jax.random.fold_in(streams_of[6], 71), 0)
    tile_lists = draw_tile_lists(jax.random.fold_in(streams_of[6], 71), 0)
    counts = place_ends(jax.random.randint(streams_of[3], (N_CELL, TILES), LIST // 2, LIST + 1), jax.random.fold_in(streams_of[3], 1), LIST // 2, LIST).astype(jnp.int32)
    cell_rank = jax.vmap(lambda own: jax.random.permutation(own, N_CELL))(jax.random.split(streams_of[4], TILES)).reshape((TILES, N_CELL)).astype(jnp.int32)
    d_colour = centred(streams_of[5], (TILES, 3, PIX), 16.0, 96.0, ((0, 64), (2, 8)), jnp.float32)
    return dict(gaussians=gaussians, fetch_ids=fetch_ids, tile_lists=tile_lists, counts=counts, cell_rank=cell_rank, d_colour=d_colour)


def render_tile(blocks, live_count):
    list_len = blocks.shape[0]
    gauss_count = blocks.shape[2]
    pixels = jnp.arange(PIX, dtype=jnp.int32)
    across = (pixels % TILE_SIDE).astype(jnp.float32) + 0.5
    pixel_row = (pixels // TILE_SIDE).astype(jnp.float32) + 0.5
    delta_x = across[None, None, :] - blocks[:, 0, :, None]
    delta_y = pixel_row[None, None, :] - blocks[:, 1, :, None]
    inverse_a = jnp.exp(blocks[:, 2, :, None])
    inverse_c = jnp.exp(blocks[:, 3, :, None])
    cross_term = blocks[:, 4, :, None] * jnp.exp(0.5 * (blocks[:, 2, :, None] + blocks[:, 3, :, None]))
    exponent = 0.5 * (inverse_a * delta_x * delta_x + inverse_c * delta_y * delta_y) + cross_term * delta_x * delta_y
    live_mask = (jnp.arange(list_len, dtype=jnp.int32) < live_count).astype(jnp.float32)
    opacity = jax.nn.sigmoid(blocks[:, 5, :]) * live_mask[:, None]
    coverage = opacity[:, :, None] * jnp.exp(-exponent)
    log_keep = jnp.log1p(-coverage)
    flat_log = log_keep.reshape(list_len * gauss_count, PIX)
    inclusive = jnp.cumsum(flat_log, axis=0)
    weight = jnp.exp(inclusive - flat_log) * coverage.reshape(list_len * gauss_count, PIX)
    colour_rows = jnp.transpose(blocks[:, 6:9, :], (1, 0, 2)).reshape(3, list_len * gauss_count)
    colour = jnp.dot(colour_rows, weight, precision=lax.Precision.HIGHEST)
    return (colour, inclusive[-1])

def reference(gaussians, fetch_ids, tile_lists, counts, cell_rank, d_colour):
    per_cell = BLK_DEV * N_OWN
    tile_owner = jnp.arange(TILES, dtype=jnp.int32) // TILE_DEV
    peer_index = tile_lists // CAP
    slot_place = tile_lists % CAP
    cell_index = jnp.arange(N_CELL, dtype=jnp.int32)
    cell_ids = fetch_ids[cell_index[:, None, None], tile_owner[None, :, None], peer_index, slot_place]
    global_ids = (cell_ids + (cell_index * per_cell)[:, None, None]).astype(jnp.int32)

    def forward(gaussian_rows):
        pair_params = gaussian_rows[global_ids.reshape(-1, LIST)]

        def render_one(tile_args):
            return render_tile(tile_args[0], tile_args[1])
        part, log_total = lax.map(jax.checkpoint(render_one), (pair_params, counts.reshape(-1)))
        part = part.reshape(N_CELL, TILES, 3, PIX)
        log_total = log_total.reshape(N_CELL, TILES, PIX)
        earlier = (cell_rank[:, None, :] < cell_rank[:, :, None]).astype(jnp.float32)
        shade_log = jnp.einsum('tab,btp->atp', earlier, log_total, precision=lax.Precision.HIGHEST)
        return jnp.einsum('atp,atkp->tkp', jnp.exp(shade_log), part, precision=lax.Precision.HIGHEST)
    image, pullback = jax.vjp(forward, gaussians)
    return (image, pullback(d_colour)[0])
```

```python
import jax
import jax.numpy as jnp
from jax import lax
from jax.experimental import pallas as pl
from jax.experimental.pallas import tpu as pltpu
from jax.sharding import PartitionSpec as P

MESH = pl.DeviceIdType.MESH
F32 = jnp.float32
BF16 = jnp.bfloat16

LIST = 12
CAP = 4
OWN = 64
CELL = 8
BLK = 8
GP = 128
NPX = 4
L_PEER, L_RANK, L_BLK, L_DCOL = 0, 16, 32, 64


def iota(shape, dim):
    return lax.broadcasted_iota(jnp.int32, shape, dim)


def split(x):
    hi = x.astype(BF16)
    return hi, (x - hi.astype(F32)).astype(BF16)


def mm(a, b):
    return lax.dot_general(a, b, (((1,), (0,)), ((), ())), preferred_element_type=F32)


def mm_nt(a, b):
    return lax.dot_general(a, b, (((1,), (1,)), ((), ())), preferred_element_type=F32)


def wait_rows(ref, rows, sem):
    view = ref.at[pl.ds(0, rows)]
    pltpu.make_async_copy(view, view, sem).wait()


def kernel(
    fetch_s, list_s, count_s, rank_s, g_ref, dcol_ref,
    colour_ref, grad_ref,
    w_ref, u_ref, wsplit_ref, wcol_ref, crow_ref, mom_ref, dpad_ref,
    fold_ref, unfold_ref, hot_ref, pick_ref, hot_t_ref, rank_ref, lit_ref, dens_ref,
    send_s, send_a, recv_s, recv_a, all_x, send_d, recv_d, send_f, recv_f, send_c, recv_c,
    send_sem, recv_sem,
):
    cell = lax.axis_index("cell")
    own = lax.axis_index("own")
    own_y = own // 8
    own_z = own % 8
    holder = own_y == cell

    barrier = pltpu.get_barrier_semaphore()

    def greet(i, carry):
        pl.semaphore_signal(barrier, inc=1, device_id=(cell, (own + i) % OWN), device_id_type=MESH)
        return carry

    lax.fori_loop(1, OWN, greet, 0)
    for i in range(1, CELL):
        pl.semaphore_signal(barrier, inc=1, device_id=((cell + i) % CELL, own), device_id_type=MESH)

    lane1 = iota((1, GP), 1)
    lane8 = iota((8, GP), 1)
    row8 = iota((8, GP), 0)
    chan8 = (lane8 % 16) // 4

    live_n = count_s[0, 0]
    aux = jnp.zeros((1, GP), jnp.int32)
    for entry in range(LIST):
        slot = list_s[0, entry]
        peer = slot // CAP
        block = fetch_s[slot % CAP, peer] - peer * BLK
        live = (entry < live_n).astype(jnp.int32)
        aux = jnp.where(lane1 == L_PEER + entry, live * (peer + 1) - 1, aux)
        aux = jnp.where(lane1 == L_BLK + entry, block, aux)
    for c in range(CELL):
        aux = jnp.where(lane1 == L_RANK + c, rank_s[0, c], aux)
    aux = jnp.broadcast_to(aux.astype(F32), (8, GP))
    dpad_ref[...] = jnp.zeros((8, GP), F32)
    for k in range(3):
        dpad_ref[k : k + 1, 0:32] = dcol_ref[k]
    slanted = pltpu.roll(dpad_ref[...], 0, 1, stride=4, stride_axis=0)
    of_row = ((lane8 - L_DCOL) // 4 == row8) & (lane8 >= L_DCOL) & (row8 < 3)
    dcol_rows = jnp.zeros((8, GP), F32)
    for i in range(8):
        moved = jnp.where(of_row, pltpu.roll(slanted, L_DCOL - 4 * i, 1), 0.0)
        moved = jnp.broadcast_to(jnp.sum(moved, axis=0, keepdims=True), (8, GP))
        dcol_rows = jnp.where(row8 == i, moved, dcol_rows)
    for i in range(8):
        mine = (cell == i).astype(F32)
        send_a[8 * i : 8 * i + 8, 0, :] = aux + mine * dcol_rows

    mean_x, mean_y = g_ref[0], g_ref[1]
    inv_a, inv_c = jnp.exp(g_ref[2]), jnp.exp(g_ref[3])
    mid = jnp.exp(0.5 * (g_ref[2] + g_ref[3]))
    cross = g_ref[4] * mid
    opacity = jax.nn.sigmoid(g_ref[5])
    crow_ref[...] = jnp.zeros((32, GP), F32)
    for k in range(3):
        crow_ref[pl.ds(k, 8, stride=4), :] = g_ref[6 + k]
    crow = crow_ref[...]
    row32 = iota((32, GP), 0)
    before_of = (iota((2 * GP, GP), 0) % GP < iota((2 * GP, GP), 1)).astype(F32).astype(BF16)
    xs = [(4 * (row8 % 4) + r).astype(F32) + 0.5 for r in range(NPX)]
    ys = (2 * iota((8, 8, GP), 0) + iota((8, 8, GP), 1) // 4).astype(F32) + 0.5

    total = jnp.zeros((256, 64), F32)
    for b in range(BLK):
        of = lambda v: jnp.broadcast_to(v[b : b + 1, :], (8, GP))
        mx, my, ca, cc, cb, op = (of(v) for v in (mean_x, mean_y, inv_a, inv_c, cross, opacity))
        dy = ys - my[None]
        part_y = (-0.5 * cc)[None] * dy * dy
        slope = cb[None] * dy
        covs = []
        for r in range(NPX):
            dx = xs[r] - mx
            covs.append(op[None] * jnp.exp(part_y - (0.5 * ca * dx * dx)[None] - dx[None] * slope))
        cov = jnp.stack(covs, axis=0).reshape(256, GP)
        keep_log = jnp.log(1.0 - cov)
        log_hi, log_lo = split(keep_log)
        before = mm(jnp.concatenate([log_hi, log_lo], axis=1), before_of)
        weight = jnp.exp(before) * cov
        w_hi, w_lo = split(weight)
        colour_b = jnp.where(row32 // 4 == b, crow, 0.0)
        ones_b = jnp.where(row32 == 4 * b + 3, 1.0, 0.0).astype(BF16)
        c_hi, c_lo = split(colour_b)
        none = jnp.zeros((32, GP), BF16)
        top = jnp.concatenate([c_hi, ones_b], axis=1)
        low = jnp.concatenate([c_lo, none], axis=1)
        wcol_ref[b] = jnp.concatenate([top, low, top, jnp.concatenate([none, none], axis=1)], axis=0)
        both = jnp.concatenate([top, low], axis=0)
        total += mm_nt(jnp.concatenate([w_hi, log_hi], axis=1), both)
        total += mm_nt(jnp.concatenate([w_lo, log_lo], axis=1), both)
        w_ref[b] = weight
        u_ref[b] = cov * jnp.exp(-keep_log)
        wsplit_ref[b] = jnp.concatenate([w_hi, w_lo], axis=1)
    total = jnp.concatenate([total, jnp.zeros((256, 64), F32)], axis=1)
    total = jnp.where(iota((256, GP), 1) < 32, total + pltpu.roll(total, 96, 1), 0.0)
    rows = total[0:64]
    for r in range(1, NPX):
        rows += pltpu.roll(total[64 * r : 64 * r + 64], 32 * r, 1)
    send_s[:, 0, :] = rows

    pl.semaphore_wait(barrier, OWN - 1 + CELL - 1)

    def spread_rows(source, target, slot):
        def one(i, carry):
            peer = (own + i) % OWN
            pltpu.make_async_remote_copy(
                source.at[peer], target.at[own], send_sem.at[slot], recv_sem.at[slot],
                device_id=(cell, peer), device_id_type=MESH,
            ).start()
            return carry

        lax.fori_loop(1, OWN, one, 0)
        target[pl.ds(own, 1)] = source[pl.ds(own, 1)]

    spread_rows(send_a, recv_a, 0)
    spread_rows(send_s, recv_s, 1)

    for a in range(8):
        lane_in = iota((GP, GP), 0)
        lane_out = iota((GP, GP), 1)
        same = (lane_out // 16 == a) & (lane_out % 4 == lane_in // 32)
        to_own = same & ((lane_out % 16) // 4 == lane_in % 4)
        to_all = same & (lane_in % 4 == 3)
        piece = jnp.concatenate([to_own.astype(F32), to_all.astype(F32)], axis=1).astype(BF16)
        fold_ref[256 * a : 256 * a + 128, :] = piece
        fold_ref[256 * a + 128 : 256 * a + 256, :] = piece
        back = (lane_in // 16 == a) & (lane_in % 4 == lane_out // 32) & ((lane_in % 16) // 4 == lane_out % 4)
        back = back.astype(F32).astype(BF16)
        unfold_ref[0:128, 128 * a : 128 * a + 128] = back
        unfold_ref[128:256, 128 * a : 128 * a + 128] = back

    wait_rows(recv_a, OWN - 1, recv_sem.at[0])
    lane8f = lane8.astype(F32)
    block8f = ((lane8 // 4) % 8).astype(F32)
    dense_d = jnp.zeros((8, GP), F32)
    dense_r = jnp.zeros((8, GP), F32)
    for a in range(8):
        tile_rows = recv_a[8 * a : 8 * a + 8, 0, :]
        here = lane8 // 16 == a
        dense_d = jnp.where(here, pltpu.roll(tile_rows, (16 * a - L_DCOL) % GP, 1), dense_d)
        dense_r = jnp.where(here, pltpu.roll(tile_rows, (16 * a - L_RANK) % GP, 1), dense_r)
        hots, picks = [], []
        for entry in range(LIST):
            peer = jnp.broadcast_to(tile_rows[:, L_PEER + entry : L_PEER + entry + 1], (8, GP))
            block = jnp.broadcast_to(tile_rows[:, L_BLK + entry : L_BLK + entry + 1], (8, GP))
            hots.append(jnp.where(peer == lane8f, 1.0, 0.0))
            picks.append(jnp.where(block == block8f, 1.0, 0.0))
        hot_ref[96 * a : 96 * a + 96, :] = jnp.concatenate(hots, axis=0)
        pick_ref[96 * a : 96 * a + 96, :] = jnp.concatenate(picks, axis=0).astype(BF16)
    dense_d = jnp.where(chan8 < 3, dense_d, 0.0)

    @pl.when(holder)
    def _():
        send_d[...] = dense_d
        recv_d[...] = dense_d
        for i in range(1, CELL):
            pltpu.make_async_remote_copy(
                send_d, recv_d, send_sem.at[2], recv_sem.at[2],
                device_id=((cell + i) % CELL, own), device_id_type=MESH,
            ).start()

    one_rank = jnp.concatenate([jnp.where(lane8 % 16 == c, dense_r, 0.0) for c in range(CELL)], axis=0)
    group = (iota((GP, GP), 0) // 16 == iota((GP, GP), 1) // 16).astype(F32).astype(BF16)
    rank_ref[...] = mm(one_rank.astype(BF16), group).reshape(8, 8, GP)

    wait_rows(recv_s, OWN - 1, recv_sem.at[1])
    s_hi, s_lo = split(recv_s[:, 0, :])
    taken = mm(hot_ref[...].astype(BF16)[:, 0:64], jnp.concatenate([s_hi, s_lo], axis=1)).astype(BF16)
    pick = pick_ref[...]
    taken = taken * jnp.concatenate([pick, pick], axis=1)
    taken = jnp.concatenate([taken[96 * a : 96 * a + 96] for a in range(8)], axis=1)
    folded = mm(taken, fold_ref[...])
    entry_c = folded[:, 0:128].reshape(LIST, 8, GP)
    entry_t = folded[:, 128:256].reshape(LIST, 8, GP)
    ahead = jnp.zeros((8, GP), F32)
    part = jnp.zeros((8, GP), F32)
    for entry in range(LIST):
        seen = jnp.exp(ahead)
        dens_ref[entry] = seen
        part += seen * entry_c[entry]
        ahead += entry_t[entry]
    all_x[cell] = jnp.where(chan8 < 3, part, ahead)
    for i in range(1, CELL):
        pltpu.make_async_remote_copy(
            all_x.at[cell], all_x.at[cell], send_sem.at[3], recv_sem.at[3],
            device_id=((cell + i) % CELL, own), device_id_type=MESH,
        ).start()

    hot_t_ref[...] = hot_ref[...].T[0:64].astype(BF16)
    ranks = [rank_ref[c] for c in range(CELL)]

    @pl.when(jnp.logical_not(holder))
    def _():
        pltpu.make_async_copy(recv_d, recv_d, recv_sem.at[2]).wait()

    wait_rows(all_x, CELL - 1, recv_sem.at[3])

    dense_d = recv_d[...]
    parts = [all_x[c] for c in range(CELL)]
    logs, dots = [], []
    for c in range(CELL):
        last = jnp.where(chan8 == 3, parts[c], 0.0)
        logs.append(last + pltpu.roll(last, 124, 1) + pltpu.roll(last, 120, 1) + pltpu.roll(last, 116, 1))
        lossy = parts[c] * dense_d
        dots.append(pltpu.roll(lossy, 4, 1) + pltpu.roll(lossy, 8, 1) + pltpu.roll(lossy, 12, 1))
    colour = jnp.zeros((8, GP), F32)
    behind = jnp.zeros((8, GP), F32)
    my_rank = rank_ref[cell]
    for c in range(CELL):
        shade = jnp.zeros((8, GP), F32)
        for other in range(CELL):
            if other != c:
                shade += jnp.where(ranks[other] < ranks[c], logs[other], 0.0)
        lit = jnp.exp(shade)
        lit_ref[c] = lit
        colour += lit * parts[c]
        behind += jnp.where(ranks[c] > my_rank, lit * dots[c], 0.0)
    d_part = dense_d * lit_ref[cell]
    grad_rows = [None] * LIST
    for entry in reversed(range(LIST)):
        d_c = dens_ref[entry] * d_part
        grad_rows[entry] = jnp.where(chan8 < 3, d_c, behind)
        lossy = d_c * entry_c[entry]
        behind = behind + (pltpu.roll(lossy, 4, 1) + pltpu.roll(lossy, 8, 1) + pltpu.roll(lossy, 12, 1))
    g_hi, g_lo = split(jnp.concatenate(grad_rows, axis=0))
    wide = mm(jnp.concatenate([g_hi, g_lo], axis=1), unfold_ref[...])
    wide = jnp.concatenate([wide[:, 128 * a : 128 * a + 128] for a in range(8)], axis=0)
    wide_hi, wide_lo = split(wide)
    wide = jnp.concatenate([wide_hi * pick, wide_lo * pick], axis=1)
    back = mm(hot_t_ref[...], wide)
    send_f[:, 0, :] = back[:, 0:128] + back[:, 128:256]
    spread_rows(send_f, recv_f, 4)

    for a in range(8):
        send_c[8 * a : 8 * a + 8, 0, :] = pltpu.roll(colour, (GP - 16 * a) % GP, 1)

    @pl.when(holder)
    def _():
        def one(i, carry):
            peer = (own + i) % OWN
            pltpu.make_async_remote_copy(
                send_c.at[peer], recv_c.at[own_z], send_sem.at[5], recv_sem.at[5],
                device_id=(cell, peer), device_id_type=MESH,
            ).start()
            return carry

        lax.fori_loop(1, OWN, one, 0)
        recv_c[pl.ds(own_z, 1)] = send_c[pl.ds(own, 1)]

    after_of = (iota((2 * GP, GP), 0) % GP > iota((2 * GP, GP), 1)).astype(F32).astype(BF16)
    wait_rows(recv_f, OWN - 1, recv_sem.at[4])
    cot = recv_f[:, 0, :]
    cot_hi = cot.astype(BF16).astype(F32)
    cot_lo = cot - cot_hi
    lane64 = iota((64, GP), 1)
    left = []
    for r in range(NPX):
        one = pltpu.roll(cot_hi, (GP - 32 * r) % GP, 1)
        two = pltpu.roll(cot_hi, (GP + 32 - 32 * r) % GP, 1)
        three = pltpu.roll(cot_lo, (GP + 64 - 32 * r) % GP, 1)
        left.append(jnp.where(lane64 < 32, one, jnp.where(lane64 < 64, two, jnp.where(lane64 < 96, three, 0.0))))
    left = jnp.concatenate(left, axis=0).astype(BF16)
    turned = jnp.concatenate([cot, jnp.zeros((64, GP), F32)], axis=0).T
    turned = jnp.concatenate(
        [
            turned[0:32] + pltpu.roll(turned[32:64], 64, 1),
            turned[64:96] + pltpu.roll(turned[96:128], 64, 1),
        ],
        axis=1,
    )
    turned = jnp.concatenate(split(turned), axis=0)
    d_colour = jnp.zeros((32, GP), F32)
    for b in range(BLK):
        of = lambda v: jnp.broadcast_to(v[b : b + 1, :], (8, GP))
        mx, my = of(mean_x), of(mean_y)
        pair = mm(left, wcol_ref[b])
        d_before = pair[:, 0:128] * w_ref[b]
        after = mm(jnp.concatenate(split(d_before), axis=1), after_of)
        flow = (d_before - (pair[:, 128:256] + after) * u_ref[b]).reshape(NPX, 8, 8, GP)
        dy = ys - my[None]
        m0 = mxs = mxx = mys = mxy = myy = jnp.zeros((8, GP), F32)
        for r in range(NPX):
            dx = xs[r] - mx
            q = flow[r]
            qy = q * dy
            s0, s1 = jnp.sum(q, axis=0), jnp.sum(qy, axis=0)
            m0 += s0
            mxs += s0 * dx
            mxx += s0 * dx * dx
            mys += s1
            mxy += s1 * dx
            myy += jnp.sum(qy * dy, axis=0)
        for i, m in enumerate((m0, mxs, mxx, mys, mxy, myy)):
            mom_ref[i, b : b + 1, :] = jnp.sum(m, axis=0, keepdims=True)
        grown = mm(turned, wsplit_ref[b])
        grown = grown[0:32, 0:128] + grown[0:32, 128:256] + grown[32:64, 0:128]
        d_colour = jnp.where(row32 // 4 == b, grown, d_colour)
    m0, mxs, mxx, mys, mxy, myy = (mom_ref[i] for i in range(6))
    grad_ref[0] = inv_a * mxs + cross * mys
    grad_ref[1] = inv_c * mys + cross * mxs
    grad_ref[2] = -0.5 * (inv_a * mxx + cross * mxy)
    grad_ref[3] = -0.5 * (inv_c * myy + cross * mxy)
    grad_ref[4] = -mid * mxy
    grad_ref[5] = (1.0 - opacity) * m0
    crow_ref[...] = d_colour
    for k in range(3):
        grad_ref[6 + k] = crow_ref[pl.ds(k, 8, stride=4), :]

    @pl.when(holder)
    def _():
        wait_rows(recv_c, 7, recv_sem.at[5])

    @pl.when(jnp.logical_not(holder))
    def _():
        wait_rows(recv_c, 8, recv_sem.at[5])

    tile = pltpu.roll(recv_c[:, 0, :], 0, 1, stride=4, stride_axis=0)
    for k in range(3):
        moved = pltpu.roll(tile, (GP - 4 * k) % GP, 1)
        moved = jnp.where(lane8 // 4 == row8, moved, 0.0)
        colour_ref[k] = jnp.sum(moved, axis=0, keepdims=True)[:, 0:32]

    for source, slot in ((send_a, 0), (send_s, 1), (send_f, 4)):
        wait_rows(source, OWN - 1, send_sem.at[slot])
    wait_rows(all_x, CELL - 1, send_sem.at[3])

    @pl.when(holder)
    def _():
        wait_rows(send_c, OWN - 1, send_sem.at[5])
        wait_rows(all_x, CELL - 1, send_sem.at[2])


def body(gaussians, fetch_ids, tile_lists, counts, cell_rank, d_colour):
    fetch = jnp.transpose(fetch_ids, (0, 1, 3, 2)).reshape(CAP, OWN)
    lists = tile_lists.reshape(1, LIST)
    params = jnp.transpose(gaussians, (1, 0, 2))
    d_rows = jnp.transpose(d_colour, (1, 0, 2))
    smem = pl.BlockSpec(memory_space=pltpu.SMEM)
    vmem = pl.BlockSpec(memory_space=pltpu.VMEM)
    row = lambda n: pltpu.VMEM((n, 1, GP), F32)
    colour, grads = pl.pallas_call(
        kernel,
        out_shape=(
            jax.ShapeDtypeStruct((3, 1, 32), F32),
            jax.ShapeDtypeStruct((9, BLK, GP), F32),
        ),
        in_specs=[smem, smem, smem, smem, vmem, vmem],
        out_specs=(vmem, vmem),
        scratch_shapes=[
            pltpu.VMEM((BLK, 256, GP), F32),
            pltpu.VMEM((BLK, 256, GP), F32),
            pltpu.VMEM((BLK, 256, 256), BF16),
            pltpu.VMEM((BLK, GP, 256), BF16),
            pltpu.VMEM((32, GP), F32),
            pltpu.VMEM((6, 8, GP), F32),
            pltpu.VMEM((8, GP), F32),
            pltpu.VMEM((2048, 256), BF16),
            pltpu.VMEM((256, 1024), BF16),
            pltpu.VMEM((768, GP), F32),
            pltpu.VMEM((768, GP), BF16),
            pltpu.VMEM((64, 768), BF16),
            pltpu.VMEM((8, 8, GP), F32),
            pltpu.VMEM((8, 8, GP), F32),
            pltpu.VMEM((LIST, 8, GP), F32),
            row(64), row(64), row(64), row(64),
            pltpu.VMEM((8, 8, GP), F32),
            pltpu.VMEM((8, GP), F32),
            pltpu.VMEM((8, GP), F32),
            row(64), row(64), row(64), row(8),
            pltpu.SemaphoreType.DMA((6,)),
            pltpu.SemaphoreType.DMA((6,)),
        ],
        compiler_params=pltpu.CompilerParams(
            collective_id=0, has_side_effects=True, vmem_limit_bytes=32 << 20
        ),
    )(fetch, lists, counts, cell_rank, params, d_rows)
    return jnp.transpose(colour, (1, 0, 2)), jnp.transpose(grads, (1, 0, 2))


def solution(mesh):
    in_specs = (
        P(("cell", "own"), None, None),
        P("cell", "own", None, None),
        P("cell", "own", None),
        P("cell", "own"),
        P("own", None),
        P("own", None, "cell"),
    )
    out_specs = (P("own", None, "cell"), P(("cell", "own"), None, None))
    return jax.shard_map(body, mesh=mesh, in_specs=in_specs, out_specs=out_specs, check_vma=False)
```

```python
import jax
import jax.numpy as jnp
from jax import lax
from jax.experimental import pallas as pl
from jax.experimental.pallas import tpu as pltpu
from jax.sharding import PartitionSpec as P

MESH = pl.DeviceIdType.MESH
F32 = jnp.float32
BF16 = jnp.bfloat16

LIST = 12
CAP = 4
OWN = 64
CELL = 8
CELL_ORDER = (4, 3, 5, 2, 6, 1, 7)
BLK = 8
GP = 128
NPX = 4
L_PEER, L_RANK, L_BLK, L_DCOL = 0, 16, 32, 64


def iota(shape, dim):
    return lax.broadcasted_iota(jnp.int32, shape, dim)


def split(x):
    hi = x.astype(BF16)
    return hi, (x - hi.astype(F32)).astype(BF16)


def mm(a, b):
    return lax.dot_general(a, b, (((1,), (0,)), ((), ())), preferred_element_type=F32)


def mm_nt(a, b):
    return lax.dot_general(a, b, (((1,), (1,)), ((), ())), preferred_element_type=F32)


def wait_rows(ref, rows, sem):
    view = ref.at[pl.ds(0, rows)]
    pltpu.make_async_copy(view, view, sem).wait()


def kernel(
    fetch_h, list_h, count_h, rank_h, g_h, dcol_h,
    colour_ref, grad_ref,
    fetch_s, list_s, count_s, rank_s, g_ref, dcol_ref, in_sem,
    w_ref, u_ref, wsplit_ref, wcol_ref, crow_ref, mom_ref, dpad_ref,
    fold_ref, unfold_ref, hot_ref, pick_ref, hot_t_ref, rank_ref, lit_ref, dens_ref,
    send_b, recv_b, all_x, send_d, recv_d, send_f, recv_f, send_c, recv_c,
    send_sem, recv_sem,
):
    cell = lax.axis_index("cell")
    own = lax.axis_index("own")
    own_y = lax.div(own, 8)
    own_z = lax.rem(own, 8)
    holder = own_y == cell

    def far_first(visit):
        def pair(k, carry):
            visit(lax.rem(own + 36 + k, OWN))
            visit(lax.rem(own + 35 - k, OWN))
            return carry

        def near(k, carry):
            visit(lax.rem(own + 7 - k, OWN))
            return carry

        lax.fori_loop(0, 28, pair, 0)
        lax.fori_loop(0, 7, near, 0)

    barrier = pltpu.get_barrier_semaphore()
    far_first(lambda peer: pl.semaphore_signal(barrier, inc=1, device_id=(cell, peer), device_id_type=MESH))
    for i in CELL_ORDER:
        pl.semaphore_signal(barrier, inc=1, device_id=(lax.rem(cell + i, CELL), own), device_id_type=MESH)
    loads = [
        pltpu.make_async_copy(source, target, in_sem.at[i])
        for i, (source, target) in enumerate(
            [(g_h, g_ref), (fetch_h, fetch_s), (list_h, list_s), (count_h, count_s), (rank_h, rank_s), (dcol_h, dcol_ref)]
        )
    ]
    for load in loads:
        load.start()

    lane1 = iota((1, GP), 1)
    lane8 = iota((8, GP), 1)
    row8 = iota((8, GP), 0)
    chan8 = (lane8 % 16) // 4

    for load in loads:
        load.wait()
    live_n = count_s[0, 0]
    aux = jnp.zeros((1, GP), jnp.int32)
    for entry in range(LIST):
        slot = list_s[0, entry]
        peer = slot // CAP
        block = fetch_s[slot % CAP, peer] - peer * BLK
        live = (entry < live_n).astype(jnp.int32)
        aux = jnp.where(lane1 == L_PEER + entry, live * (peer + 1) - 1, aux)
        aux = jnp.where(lane1 == L_BLK + entry, block, aux)
    for c in range(CELL):
        aux = jnp.where(lane1 == L_RANK + c, rank_s[0, c], aux)
    aux = jnp.broadcast_to(aux.astype(F32), (8, GP))
    dpad_ref[...] = jnp.zeros((8, GP), F32)
    for k in range(3):
        dpad_ref[k : k + 1, 0:32] = dcol_ref[k]
    slanted = pltpu.roll(dpad_ref[...], 0, 1, stride=4, stride_axis=0)
    of_row = ((lane8 - L_DCOL) // 4 == row8) & (lane8 >= L_DCOL) & (row8 < 3)
    dcol_rows = jnp.zeros((8, GP), F32)
    for i in range(8):
        moved = jnp.where(of_row, pltpu.roll(slanted, L_DCOL - 4 * i, 1), 0.0)
        moved = jnp.broadcast_to(jnp.sum(moved, axis=0, keepdims=True), (8, GP))
        dcol_rows = jnp.where(row8 == i, moved, dcol_rows)
    for i in range(8):
        mine = (cell == i).astype(F32)
        send_b[pl.ds(16 * i + 1, 8, stride=2), :] = aux + mine * dcol_rows

    mean_x, mean_y = g_ref[0], g_ref[1]
    inv_a, inv_c = jnp.exp(g_ref[2]), jnp.exp(g_ref[3])
    mid = jnp.exp(0.5 * (g_ref[2] + g_ref[3]))
    cross = g_ref[4] * mid
    opacity = jax.nn.sigmoid(g_ref[5])
    crow_ref[...] = jnp.zeros((32, GP), F32)
    for k in range(3):
        crow_ref[pl.ds(k, 8, stride=4), :] = g_ref[6 + k]
    crow = crow_ref[...]
    row32 = iota((32, GP), 0)
    before_of = (iota((2 * GP, GP), 0) % GP < iota((2 * GP, GP), 1)).astype(F32).astype(BF16)
    xs = [(4 * (row8 % 4) + r).astype(F32) + 0.5 for r in range(NPX)]
    ys = (2 * iota((8, 8, GP), 0) + iota((8, 8, GP), 1) // 4).astype(F32) + 0.5

    total = jnp.zeros((256, 64), F32)
    for b in range(BLK):
        of = lambda v: jnp.broadcast_to(v[b : b + 1, :], (8, GP))
        mx, my, ca, cc, cb, op = (of(v) for v in (mean_x, mean_y, inv_a, inv_c, cross, opacity))
        dy = ys - my[None]
        part_y = (-0.5 * cc)[None] * dy * dy
        slope = cb[None] * dy
        covs = []
        for r in range(NPX):
            dx = xs[r] - mx
            covs.append(op[None] * jnp.exp(part_y - (0.5 * ca * dx * dx)[None] - dx[None] * slope))
        cov = jnp.stack(covs, axis=0).reshape(256, GP)
        keep_log = jnp.log(1.0 - cov)
        log_hi, log_lo = split(keep_log)
        before = mm(jnp.concatenate([log_hi, log_lo], axis=1), before_of)
        weight = jnp.exp(before) * cov
        w_hi, w_lo = split(weight)
        colour_b = jnp.where(row32 // 4 == b, crow, 0.0)
        ones_b = jnp.where(row32 == 4 * b + 3, 1.0, 0.0).astype(BF16)
        c_hi, c_lo = split(colour_b)
        none = jnp.zeros((32, GP), BF16)
        top = jnp.concatenate([c_hi, ones_b], axis=1)
        low = jnp.concatenate([c_lo, none], axis=1)
        wcol_ref[b] = jnp.concatenate([top, low, top, jnp.concatenate([none, none], axis=1)], axis=0)
        both = jnp.concatenate([top, low], axis=0)
        total += mm_nt(jnp.concatenate([w_hi, log_hi], axis=1), both)
        total += mm_nt(jnp.concatenate([w_lo, log_lo], axis=1), both)
        w_ref[b] = weight
        u_ref[b] = cov * jnp.exp(-keep_log)
        wsplit_ref[b] = jnp.concatenate([w_hi, w_lo], axis=1)
    total = jnp.concatenate([total, jnp.zeros((256, 64), F32)], axis=1)
    total = jnp.where(iota((256, GP), 1) < 32, total + pltpu.roll(total, 96, 1), 0.0)
    rows = total[0:64]
    for r in range(1, NPX):
        rows += pltpu.roll(total[64 * r : 64 * r + 64], 32 * r, 1)
    send_b[pl.ds(0, 64, stride=2), :] = rows

    pl.semaphore_wait(barrier, OWN - 1 + CELL - 1)

    def spread_rows(source, target, rows, slot):
        def one(peer):
            pltpu.make_async_remote_copy(
                source.at[pl.ds(rows * peer, rows)], target.at[pl.ds(rows * own, rows)],
                send_sem.at[slot], recv_sem.at[slot], device_id=(cell, peer), device_id_type=MESH,
            ).start()

        far_first(one)
        for i in range(rows):
            target[pl.ds(rows * own + i, 1), :] = source[pl.ds(rows * own + i, 1), :]

    spread_rows(send_b, recv_b, 2, 0)

    for a in range(8):
        lane_in = iota((GP, GP), 0)
        lane_out = iota((GP, GP), 1)
        same = (lane_out // 16 == a) & (lane_out % 4 == lane_in // 32)
        to_own = same & ((lane_out % 16) // 4 == lane_in % 4)
        to_all = same & (lane_in % 4 == 3)
        piece = jnp.concatenate([to_own.astype(F32), to_all.astype(F32)], axis=1).astype(BF16)
        fold_ref[256 * a : 256 * a + 128, :] = piece
        fold_ref[256 * a + 128 : 256 * a + 256, :] = piece
        back = (lane_in // 16 == a) & (lane_in % 4 == lane_out // 32) & ((lane_in % 16) // 4 == lane_out % 4)
        back = back.astype(F32).astype(BF16)
        unfold_ref[0:128, 128 * a : 128 * a + 128] = back
        unfold_ref[128:256, 128 * a : 128 * a + 128] = back

    choose_in = iota((GP, 256), 0)
    choose_out = iota((GP, 256), 1)
    choose = (choose_in < 16) & (choose_out < 128) | (choose_in >= 32) & (choose_in < 48) & (choose_out >= 128)
    choose = choose.astype(F32).astype(BF16)
    wait_rows(recv_b, 2 * (OWN - 1), recv_sem.at[0])
    lane8f = lane8.astype(F32)
    block8f = ((lane8 // 4) % 8).astype(F32)
    dense_d = jnp.zeros((8, GP), F32)
    dense_r = jnp.zeros((8, GP), F32)
    lone = []
    for a in range(8):
        tile_rows = recv_b[pl.ds(16 * a + 1, 8, stride=2), :]
        here = lane8 // 16 == a
        dense_d = jnp.where(here, pltpu.roll(tile_rows, (16 * a - L_DCOL) % GP, 1), dense_d)
        dense_r = jnp.where(here, pltpu.roll(tile_rows, (16 * a - L_RANK) % GP, 1), dense_r)
        for entry in range(LIST):
            mine = (lane8 == L_PEER + entry) | (lane8 == L_BLK + entry)
            lone.append(jnp.where(mine, tile_rows, 0.0))
    named = mm(jnp.concatenate(lone, axis=0).astype(BF16), choose).reshape(96, 8, 256)
    hot = jnp.where(named[:, :, 0:128] == lane8f[None], 1.0, 0.0).reshape(768, GP)
    pick = jnp.where(named[:, :, 128:256] == block8f[None], 1.0, 0.0).reshape(768, GP).astype(BF16)
    hot_ref[...] = hot
    pick_ref[...] = pick
    dense_d = jnp.where(chan8 < 3, dense_d, 0.0)

    @pl.when(holder)
    def _():
        send_d[...] = dense_d
        recv_d[...] = dense_d
        for i in CELL_ORDER:
            pltpu.make_async_remote_copy(
                send_d, recv_d, send_sem.at[2], recv_sem.at[2],
                device_id=(lax.rem(cell + i, CELL), own), device_id_type=MESH,
            ).start()

    one_rank = jnp.concatenate([jnp.where(lane8 % 16 == c, dense_r, 0.0) for c in range(CELL)], axis=0)
    group = (iota((GP, GP), 0) // 16 == iota((GP, GP), 1) // 16).astype(F32).astype(BF16)
    rank_ref[...] = mm(one_rank.astype(BF16), group).reshape(8, 8, GP)

    s_hi, s_lo = split(recv_b[pl.ds(0, 64, stride=2), :])
    taken = mm(hot.astype(BF16)[:, 0:64], jnp.concatenate([s_hi, s_lo], axis=1)).astype(BF16)
    taken = taken * jnp.concatenate([pick, pick], axis=1)
    taken = jnp.concatenate([taken[96 * a : 96 * a + 96] for a in range(8)], axis=1)
    folded = mm(taken, fold_ref[...])
    entry_c = folded[:, 0:128].reshape(LIST, 8, GP)
    entry_t = folded[:, 128:256].reshape(LIST, 8, GP)
    ahead = jnp.zeros((8, GP), F32)
    part = jnp.zeros((8, GP), F32)
    for entry in range(LIST):
        seen = jnp.exp(ahead)
        dens_ref[entry] = seen
        part += seen * entry_c[entry]
        ahead += entry_t[entry]
    all_x[cell] = jnp.where(chan8 < 3, part, ahead)
    for i in CELL_ORDER:
        pltpu.make_async_remote_copy(
            all_x.at[cell], all_x.at[cell], send_sem.at[3], recv_sem.at[3],
            device_id=(lax.rem(cell + i, CELL), own), device_id_type=MESH,
        ).start()

    hot_t_ref[...] = hot_ref[...].T[0:64].astype(BF16)
    ranks = [rank_ref[c] for c in range(CELL)]

    @pl.when(jnp.logical_not(holder))
    def _():
        pltpu.make_async_copy(recv_d, recv_d, recv_sem.at[2]).wait()

    wait_rows(all_x, CELL - 1, recv_sem.at[3])

    dense_d = recv_d[...]
    parts = [all_x[c] for c in range(CELL)]
    logs, dots = [], []
    for c in range(CELL):
        last = jnp.where(chan8 == 3, parts[c], 0.0)
        logs.append(last + pltpu.roll(last, 124, 1) + pltpu.roll(last, 120, 1) + pltpu.roll(last, 116, 1))
        lossy = parts[c] * dense_d
        dots.append(pltpu.roll(lossy, 4, 1) + pltpu.roll(lossy, 8, 1) + pltpu.roll(lossy, 12, 1))
    colour = jnp.zeros((8, GP), F32)
    behind = jnp.zeros((8, GP), F32)
    my_rank = rank_ref[cell]
    for c in range(CELL):
        shade = jnp.zeros((8, GP), F32)
        for other in range(CELL):
            if other != c:
                shade += jnp.where(ranks[other] < ranks[c], logs[other], 0.0)
        lit = jnp.exp(shade)
        lit_ref[c] = lit
        colour += lit * parts[c]
        behind += jnp.where(ranks[c] > my_rank, lit * dots[c], 0.0)
    d_part = dense_d * lit_ref[cell]
    grad_rows = [None] * LIST
    for entry in reversed(range(LIST)):
        d_c = dens_ref[entry] * d_part
        grad_rows[entry] = jnp.where(chan8 < 3, d_c, behind)
        lossy = d_c * entry_c[entry]
        behind = behind + (pltpu.roll(lossy, 4, 1) + pltpu.roll(lossy, 8, 1) + pltpu.roll(lossy, 12, 1))
    pick = pick_ref[...]
    g_hi, g_lo = split(jnp.concatenate(grad_rows, axis=0))
    wide = mm(jnp.concatenate([g_hi, g_lo], axis=1), unfold_ref[...])
    wide = jnp.concatenate([wide[:, 128 * a : 128 * a + 128] for a in range(8)], axis=0)
    wide_hi, wide_lo = split(wide)
    wide = jnp.concatenate([wide_hi * pick, wide_lo * pick], axis=1)
    back = mm(hot_t_ref[...], wide)
    send_f[...] = back[:, 0:128] + back[:, 128:256]
    spread_rows(send_f, recv_f, 1, 4)

    for a in range(8):
        send_c[8 * a : 8 * a + 8, :] = pltpu.roll(colour, (GP - 16 * a) % GP, 1)

    @pl.when(holder)
    def _():
        far_first(
            lambda peer: pltpu.make_async_remote_copy(
                send_c.at[pl.ds(peer, 1)], recv_c.at[pl.ds(own_z, 1)], send_sem.at[5], recv_sem.at[5],
                device_id=(cell, peer), device_id_type=MESH,
            ).start()
        )
        recv_c[pl.ds(own_z, 1), :] = send_c[pl.ds(own, 1), :]

    after_of = (iota((2 * GP, GP), 0) % GP > iota((2 * GP, GP), 1)).astype(F32).astype(BF16)
    wait_rows(recv_f, OWN - 1, recv_sem.at[4])
    cot = recv_f[...]
    cot_hi = cot.astype(BF16).astype(F32)
    cot_lo = cot - cot_hi
    lane64 = iota((64, GP), 1)
    left = []
    for r in range(NPX):
        one = pltpu.roll(cot_hi, (GP - 32 * r) % GP, 1)
        two = pltpu.roll(cot_hi, (GP + 32 - 32 * r) % GP, 1)
        three = pltpu.roll(cot_lo, (GP + 64 - 32 * r) % GP, 1)
        left.append(jnp.where(lane64 < 32, one, jnp.where(lane64 < 64, two, jnp.where(lane64 < 96, three, 0.0))))
    left = jnp.concatenate(left, axis=0).astype(BF16)
    turned = jnp.concatenate([cot, jnp.zeros((64, GP), F32)], axis=0).T
    turned = jnp.concatenate(
        [
            turned[0:32] + pltpu.roll(turned[32:64], 64, 1),
            turned[64:96] + pltpu.roll(turned[96:128], 64, 1),
        ],
        axis=1,
    )
    turned = jnp.concatenate(split(turned), axis=0)
    d_colour = jnp.zeros((32, GP), F32)
    for b in range(BLK):
        of = lambda v: jnp.broadcast_to(v[b : b + 1, :], (8, GP))
        mx, my = of(mean_x), of(mean_y)
        pair = mm(left, wcol_ref[b])
        d_before = pair[:, 0:128] * w_ref[b]
        after = mm(jnp.concatenate(split(d_before), axis=1), after_of)
        flow = (d_before - (pair[:, 128:256] + after) * u_ref[b]).reshape(NPX, 8, 8, GP)
        dy = ys - my[None]
        m0 = mxs = mxx = mys = mxy = myy = jnp.zeros((8, GP), F32)
        for r in range(NPX):
            dx = xs[r] - mx
            q = flow[r]
            qy = q * dy
            s0, s1 = jnp.sum(q, axis=0), jnp.sum(qy, axis=0)
            m0 += s0
            mxs += s0 * dx
            mxx += s0 * dx * dx
            mys += s1
            mxy += s1 * dx
            myy += jnp.sum(qy * dy, axis=0)
        for i, m in enumerate((m0, mxs, mxx, mys, mxy, myy)):
            mom_ref[i, b : b + 1, :] = jnp.sum(m, axis=0, keepdims=True)
        grown = mm(turned, wsplit_ref[b])
        grown = grown[0:32, 0:128] + grown[0:32, 128:256] + grown[32:64, 0:128]
        d_colour = jnp.where(row32 // 4 == b, grown, d_colour)
    m0, mxs, mxx, mys, mxy, myy = (mom_ref[i] for i in range(6))
    grad_ref[0] = inv_a * mxs + cross * mys
    grad_ref[1] = inv_c * mys + cross * mxs
    grad_ref[2] = -0.5 * (inv_a * mxx + cross * mxy)
    grad_ref[3] = -0.5 * (inv_c * myy + cross * mxy)
    grad_ref[4] = -mid * mxy
    grad_ref[5] = (1.0 - opacity) * m0
    crow_ref[...] = d_colour
    for k in range(3):
        grad_ref[6 + k] = crow_ref[pl.ds(k, 8, stride=4), :]

    @pl.when(holder)
    def _():
        wait_rows(recv_c, 7, recv_sem.at[5])

    @pl.when(jnp.logical_not(holder))
    def _():
        wait_rows(recv_c, 8, recv_sem.at[5])

    tile = pltpu.roll(recv_c[...], 0, 1, stride=4, stride_axis=0)
    for k in range(3):
        moved = pltpu.roll(tile, (GP - 4 * k) % GP, 1)
        moved = jnp.where(lane8 // 4 == row8, moved, 0.0)
        colour_ref[k] = jnp.sum(moved, axis=0, keepdims=True)[:, 0:32]

    wait_rows(send_b, 2 * (OWN - 1), send_sem.at[0])
    wait_rows(send_f, OWN - 1, send_sem.at[4])
    wait_rows(all_x, CELL - 1, send_sem.at[3])

    @pl.when(holder)
    def _():
        wait_rows(send_c, OWN - 1, send_sem.at[5])
        wait_rows(all_x, CELL - 1, send_sem.at[2])


def put(colour_ref, grad_ref, colour_out, grad_out, sem):
    one = pltpu.make_async_copy(colour_ref, colour_out, sem.at[0])
    two = pltpu.make_async_copy(grad_ref, grad_out, sem.at[1])
    two.start()
    one.start()
    two.wait()
    one.wait()


def finish(colour, grads):
    vmem = pl.BlockSpec(memory_space=pltpu.VMEM)
    hbm = pl.BlockSpec(memory_space=pltpu.HBM)
    return pl.pallas_call(
        put,
        out_shape=(jax.ShapeDtypeStruct(colour.shape, F32), jax.ShapeDtypeStruct(grads.shape, F32)),
        in_specs=[vmem, vmem],
        out_specs=(hbm, hbm),
        scratch_shapes=[pltpu.SemaphoreType.DMA((2,))],
        compiler_params=pltpu.CompilerParams(vmem_limit_bytes=1 << 20),
    )(colour, grads)


def body(gaussians, fetch_ids, tile_lists, counts, cell_rank, d_colour):
    fetch = jnp.transpose(fetch_ids, (0, 1, 3, 2)).reshape(CAP, OWN)
    lists = tile_lists.reshape(1, LIST)
    hb = lambda v: pltpu.with_memory_space_constraint(v, pltpu.HBM)
    params = jnp.transpose(gaussians, (1, 0, 2))
    d_rows = jnp.transpose(d_colour, (1, 0, 2))
    hbm = pl.BlockSpec(memory_space=pltpu.HBM)
    vmem = pl.BlockSpec(memory_space=pltpu.VMEM)
    row = lambda n: pltpu.VMEM((n, GP), F32)
    colour, grads = pl.pallas_call(
        kernel,
        out_shape=(
            jax.ShapeDtypeStruct((3, 1, 32), F32),
            jax.ShapeDtypeStruct((9, BLK, GP), F32),
        ),
        in_specs=[hbm] * 6,
        out_specs=(vmem, vmem),
        scratch_shapes=[
            pltpu.SMEM((CAP, OWN), jnp.int32),
            pltpu.SMEM((1, LIST), jnp.int32),
            pltpu.SMEM((1, 1), jnp.int32),
            pltpu.SMEM((1, CELL), jnp.int32),
            pltpu.VMEM((9, BLK, GP), F32),
            pltpu.VMEM((3, 1, 32), F32),
            pltpu.SemaphoreType.DMA((6,)),
            pltpu.VMEM((BLK, 256, GP), F32),
            pltpu.VMEM((BLK, 256, GP), F32),
            pltpu.VMEM((BLK, 256, 256), BF16),
            pltpu.VMEM((BLK, GP, 256), BF16),
            pltpu.VMEM((32, GP), F32),
            pltpu.VMEM((6, 8, GP), F32),
            pltpu.VMEM((8, GP), F32),
            pltpu.VMEM((2048, 256), BF16),
            pltpu.VMEM((256, 1024), BF16),
            pltpu.VMEM((768, GP), F32),
            pltpu.VMEM((768, GP), BF16),
            pltpu.VMEM((64, 768), BF16),
            pltpu.VMEM((8, 8, GP), F32),
            pltpu.VMEM((8, 8, GP), F32),
            pltpu.VMEM((LIST, 8, GP), F32),
            row(128), row(128),
            pltpu.VMEM((8, 8, GP), F32),
            pltpu.VMEM((8, GP), F32),
            pltpu.VMEM((8, GP), F32),
            row(64), row(64), row(64), row(8),
            pltpu.SemaphoreType.DMA((6,)),
            pltpu.SemaphoreType.DMA((6,)),
        ],
        compiler_params=pltpu.CompilerParams(
            collective_id=0, has_side_effects=True, vmem_limit_bytes=32 << 20
        ),
    )(hb(fetch), hb(lists), counts, hb(cell_rank), hb(params), hb(d_rows))
    colour, grads = finish(colour, grads)
    return jnp.transpose(colour, (1, 0, 2)), jnp.transpose(grads, (1, 0, 2))


def solution(mesh):
    in_specs = (
        P(("cell", "own"), None, None),
        P("cell", "own", None, None),
        P("cell", "own", None),
        P("cell", "own"),
        P("own", None),
        P("own", None, "cell"),
    )
    out_specs = (P("own", None, "cell"), P(("cell", "own"), None, None))
    return jax.shard_map(body, mesh=mesh, in_specs=in_specs, out_specs=out_specs, check_vma=False)
```

```python
import jax
import jax.numpy as jnp
from jax import lax
from jax.experimental import pallas as pl
from jax.experimental.pallas import tpu as pltpu
from jax.sharding import PartitionSpec as P

MESH = pl.DeviceIdType.MESH
F32 = jnp.float32
BF16 = jnp.bfloat16

LIST = 12
CAP = 4
OWN = 64
CELL = 8
CELL_ORDER = (4, 3, 5, 2, 6, 1, 7)
BLK = 8
GP = 128
NPX = 4
HEADS = 32
HALVES = 2
L_PEER, L_RANK, L_BLK, L_DCOL = 0, 16, 32, 64


def iota(shape, dim):
    return lax.broadcasted_iota(jnp.int32, shape, dim)


def split(x):
    hi = x.astype(BF16)
    return hi, (x - hi.astype(F32)).astype(BF16)


def mm(a, b):
    return lax.dot_general(a, b, (((1,), (0,)), ((), ())), preferred_element_type=F32)


def mm_nt(a, b):
    return lax.dot_general(a, b, (((1,), (1,)), ((), ())), preferred_element_type=F32)


def wait_rows(ref, rows, sem):
    view = ref.at[pl.ds(0, rows)]
    pltpu.make_async_copy(view, view, sem).wait()


def kernel(
    fetch_h, list_h, count_h, rank_h, g_h, dcol_h,
    colour_ref, grad_ref,
    fetch_s, list_s, count_s, rank_s, g_ref, dcol_ref, in_sem,
    w_ref, u_ref, wsplit_ref, wcol_ref, crow_ref, mom_ref, dpad_ref, rows_ref,
    fold_ref, unfold_ref, hot_ref, pick_ref, hot_t_ref, rank_ref, lit_ref, dens_ref,
    send_b, recv_b, all_x, send_d, recv_d, send_f, recv_f, send_c, recv_c,
    send_sem, recv_sem,
):
    cell = lax.axis_index("cell")
    own = lax.axis_index("own")
    own_y = lax.div(own, 8)
    own_z = lax.rem(own, 8)
    head = own_z < 4
    not_head = own_z >= 4
    pair_of = 4 * own_y + own_z
    holder = head & (own_y == cell)

    def far_first(visit):
        def pair(k, carry):
            visit(lax.rem(own + 36 + k, OWN))
            visit(lax.rem(own + 35 - k, OWN))
            return carry

        def near(k, carry):
            visit(lax.rem(own + 7 - k, OWN))
            return carry

        lax.fori_loop(0, 28, pair, 0)
        lax.fori_loop(0, 7, near, 0)

    barrier = pltpu.get_barrier_semaphore()

    @pl.when(head)
    def _():
        far_first(lambda peer: pl.semaphore_signal(barrier, inc=1, device_id=(cell, peer), device_id_type=MESH))
        for i in CELL_ORDER:
            pl.semaphore_signal(barrier, inc=1, device_id=(lax.rem(cell + i, CELL), own), device_id_type=MESH)

    loads = [
        pltpu.make_async_copy(source, target, in_sem.at[i])
        for i, (source, target) in enumerate(
            [(g_h, g_ref), (fetch_h, fetch_s), (list_h, list_s), (count_h, count_s), (rank_h, rank_s), (dcol_h, dcol_ref)]
        )
    ]
    for load in loads:
        load.start()

    lane1 = iota((1, GP), 1)
    lane8 = iota((8, GP), 1)
    row8 = iota((8, GP), 0)
    chan8 = (lane8 % 16) // 4

    for load in loads:
        load.wait()
    live_n = count_s[0, 0]
    aux = jnp.zeros((1, GP), jnp.int32)
    for entry in range(LIST):
        slot = list_s[0, entry]
        peer = slot // CAP
        block = fetch_s[slot % CAP, peer] - peer * BLK
        live = (entry < live_n).astype(jnp.int32)
        aux = jnp.where(lane1 == L_PEER + entry, live * (peer + 1) - 1, aux)
        aux = jnp.where(lane1 == L_BLK + entry, block, aux)
    for c in range(CELL):
        aux = jnp.where(lane1 == L_RANK + c, rank_s[0, c], aux)
    aux = jnp.broadcast_to(aux.astype(F32), (8, GP))
    dpad_ref[...] = jnp.zeros((8, GP), F32)
    for k in range(3):
        dpad_ref[k : k + 1, 0:32] = dcol_ref[k]
    slanted = pltpu.roll(dpad_ref[...], 0, 1, stride=4, stride_axis=0)
    of_row = ((lane8 - L_DCOL) // 4 == row8) & (lane8 >= L_DCOL) & (row8 < 3)
    dcol_rows = jnp.zeros((8, GP), F32)
    for i in range(8):
        moved = jnp.where(of_row, pltpu.roll(slanted, L_DCOL - 4 * i, 1), 0.0)
        moved = jnp.broadcast_to(jnp.sum(moved, axis=0, keepdims=True), (8, GP))
        dcol_rows = jnp.where(row8 == i, moved, dcol_rows)
    rows_ref[0:8, :] = dcol_rows
    two_groups = rows_ref[pl.ds(0, 4, stride=2), :] + pltpu.roll(rows_ref[pl.ds(1, 4, stride=2), :], 16, 1)
    for i in range(8):
        mine = (cell == i).astype(F32)
        send_b[pl.ds(16 * i + 2, 4, stride=4), :] = aux[0:4] + mine * two_groups

    mean_x, mean_y = g_ref[0], g_ref[1]
    inv_a, inv_c = jnp.exp(g_ref[2]), jnp.exp(g_ref[3])
    mid = jnp.exp(0.5 * (g_ref[2] + g_ref[3]))
    cross = g_ref[4] * mid
    opacity = jax.nn.sigmoid(g_ref[5])
    crow_ref[...] = jnp.zeros((32, GP), F32)
    for k in range(3):
        crow_ref[pl.ds(k, 8, stride=4), :] = g_ref[6 + k]
    crow = crow_ref[...]
    row32 = iota((32, GP), 0)
    before_of = (iota((2 * GP, GP), 0) % GP < iota((2 * GP, GP), 1)).astype(F32).astype(BF16)
    xs = [(4 * (row8 % 4) + r).astype(F32) + 0.5 for r in range(NPX)]
    ys = (2 * iota((8, 8, GP), 0) + iota((8, 8, GP), 1) // 4).astype(F32) + 0.5

    total = jnp.zeros((256, 64), F32)
    for b in range(BLK):
        of = lambda v: jnp.broadcast_to(v[b : b + 1, :], (8, GP))
        mx, my, ca, cc, cb, op = (of(v) for v in (mean_x, mean_y, inv_a, inv_c, cross, opacity))
        dy = ys - my[None]
        part_y = (-0.5 * cc)[None] * dy * dy
        slope = cb[None] * dy
        covs = []
        for r in range(NPX):
            dx = xs[r] - mx
            covs.append(op[None] * jnp.exp(part_y - (0.5 * ca * dx * dx)[None] - dx[None] * slope))
        cov = jnp.stack(covs, axis=0).reshape(256, GP)
        keep_log = jnp.log(1.0 - cov)
        log_hi, log_lo = split(keep_log)
        before = mm(jnp.concatenate([log_hi, log_lo], axis=1), before_of)
        weight = jnp.exp(before) * cov
        w_hi, w_lo = split(weight)
        colour_b = jnp.where(row32 // 4 == b, crow, 0.0)
        ones_b = jnp.where(row32 == 4 * b + 3, 1.0, 0.0).astype(BF16)
        c_hi, c_lo = split(colour_b)
        none = jnp.zeros((32, GP), BF16)
        top = jnp.concatenate([c_hi, ones_b], axis=1)
        low = jnp.concatenate([c_lo, none], axis=1)
        wcol_ref[b] = jnp.concatenate([top, low, top, jnp.concatenate([none, none], axis=1)], axis=0)
        both = jnp.concatenate([top, low], axis=0)
        total += mm_nt(jnp.concatenate([w_hi, log_hi], axis=1), both)
        total += mm_nt(jnp.concatenate([w_lo, log_lo], axis=1), both)
        w_ref[b] = weight
        u_ref[b] = cov * jnp.exp(-keep_log)
        wsplit_ref[b] = jnp.concatenate([w_hi, w_lo], axis=1)
    total = jnp.concatenate([total, jnp.zeros((256, 64), F32)], axis=1)
    total = jnp.where(iota((256, GP), 1) < 32, total + pltpu.roll(total, 96, 1), 0.0)
    rows = total[0:64]
    for r in range(1, NPX):
        rows += pltpu.roll(total[64 * r : 64 * r + 64], 32 * r, 1)
    rows_ref[...] = rows
    for h in range(HALVES):
        send_b[pl.ds(h, HEADS, stride=4), :] = rows_ref[pl.ds(h, HEADS, stride=2), :]

    pl.semaphore_wait(barrier, jnp.where(head, HEADS - 1 + CELL - 1, HEADS))

    def to_head(pair):
        peer = pair + 4 * lax.div(pair, 4)

        @pl.when(peer != own)
        def _():
            pltpu.make_async_remote_copy(
                send_b.at[pl.ds(4 * pair, 3)], recv_b.at[pl.ds(4 * own, 3)], send_sem.at[0], recv_sem.at[0],
                device_id=(cell, peer), device_id_type=MESH,
            ).start()

    def to_two_heads(k, carry):
        to_head(lax.rem(4 * own_y + 16 + k, HEADS))
        to_head(lax.rem(4 * own_y + 47 - k, HEADS))
        return carry

    lax.fori_loop(0, HEADS // 2, to_two_heads, 0)

    def composite():
        for a in range(8):
            lane_in = iota((GP, GP), 0)
            lane_out = iota((GP, GP), 1)
            same = (lane_out // 16 == a) & (lane_out % 4 == lane_in // 32)
            to_own = same & ((lane_out % 16) // 4 == lane_in % 4)
            to_all = same & (lane_in % 4 == 3)
            piece = jnp.concatenate([to_own.astype(F32), to_all.astype(F32)], axis=1).astype(BF16)
            fold_ref[256 * a : 256 * a + 128, :] = piece
            fold_ref[256 * a + 128 : 256 * a + 256, :] = piece
            back = (lane_in // 16 == a) & (lane_in % 4 == lane_out // 32) & ((lane_in % 16) // 4 == lane_out % 4)
            back = back.astype(F32).astype(BF16)
            unfold_ref[0:128, 128 * a : 128 * a + 128] = back
            unfold_ref[128:256, 128 * a : 128 * a + 128] = back

        choose_in = iota((GP, 256), 0)
        choose_out = iota((GP, 256), 1)
        choose = (choose_in < 16) & (choose_out < 128) | (choose_in >= 32) & (choose_in < 48) & (choose_out >= 128)
        choose = choose.astype(F32).astype(BF16)
        for i in range(3):
            recv_b[pl.ds(4 * own + i, 1), :] = send_b[pl.ds(4 * pair_of + i, 1), :]
        wait_rows(recv_b, 3 * (OWN - 1), recv_sem.at[0])
        lane8f = lane8.astype(F32)
        block8f = ((lane8 // 4) % 8).astype(F32)
        dense_d = [jnp.zeros((8, GP), F32)] * HALVES
        dense_r = jnp.zeros((8, GP), F32)
        lone = []
        for a in range(8):
            tile_rows = recv_b[pl.ds(32 * a + 2, 8, stride=4), :]
            here = lane8 // 16 == a
            dense_d = [
                jnp.where(here, pltpu.roll(tile_rows, (16 * a - L_DCOL - 16 * h) % GP, 1), dense_d[h]) for h in range(HALVES)
            ]
            dense_r = jnp.where(here, pltpu.roll(tile_rows, (16 * a - L_RANK) % GP, 1), dense_r)
            for entry in range(LIST):
                mine = (lane8 == L_PEER + entry) | (lane8 == L_BLK + entry)
                lone.append(jnp.where(mine, tile_rows, 0.0))
        named = mm(jnp.concatenate(lone, axis=0).astype(BF16), choose).reshape(96, 8, 256)
        hot = jnp.where(named[:, :, 0:128] == lane8f[None], 1.0, 0.0).reshape(768, GP)
        pick = jnp.where(named[:, :, 128:256] == block8f[None], 1.0, 0.0).reshape(768, GP).astype(BF16)
        hot_ref[...] = hot
        pick_ref[...] = pick
        dense_d = [jnp.where(chan8 < 3, dense_d[h], 0.0) for h in range(HALVES)]

        @pl.when(holder)
        def _():
            for h in range(HALVES):
                send_d[h] = dense_d[h]
                recv_d[h] = dense_d[h]
            for i in CELL_ORDER:
                pltpu.make_async_remote_copy(
                    send_d, recv_d, send_sem.at[2], recv_sem.at[2],
                    device_id=(lax.rem(cell + i, CELL), own), device_id_type=MESH,
                ).start()

        one_rank = jnp.concatenate([jnp.where(lane8 % 16 == c, dense_r, 0.0) for c in range(CELL)], axis=0)
        group = (iota((GP, GP), 0) // 16 == iota((GP, GP), 1) // 16).astype(F32).astype(BF16)
        rank_ref[...] = mm(one_rank.astype(BF16), group).reshape(8, 8, GP)

        pieces = []
        for h in range(HALVES):
            pieces += split(recv_b[pl.ds(h, 64, stride=4), :])
        taken = mm(hot.astype(BF16)[:, 0:64], jnp.concatenate(pieces, axis=1)).astype(BF16)
        taken = taken * jnp.concatenate([pick] * 4, axis=1)
        taken = jnp.concatenate(
            [
                jnp.concatenate([taken[96 * a : 96 * a + 96, 256 * h : 256 * h + 256] for a in range(8)], axis=1)
                for h in range(HALVES)
            ],
            axis=0,
        )
        folded = mm(taken, fold_ref[...])
        entry_c = folded[:, 0:128].reshape(HALVES, LIST, 8, GP)
        entry_t = folded[:, 128:256].reshape(HALVES, LIST, 8, GP)
        for h in range(HALVES):
            ahead = jnp.zeros((8, GP), F32)
            part = jnp.zeros((8, GP), F32)
            for entry in range(LIST):
                seen = jnp.exp(ahead)
                dens_ref[h, entry] = seen
                part += seen * entry_c[h, entry]
                ahead += entry_t[h, entry]
            all_x[cell, h] = jnp.where(chan8 < 3, part, ahead)
        for i in CELL_ORDER:
            pltpu.make_async_remote_copy(
                all_x.at[cell], all_x.at[cell], send_sem.at[3], recv_sem.at[3],
                device_id=(lax.rem(cell + i, CELL), own), device_id_type=MESH,
            ).start()

        hot_t_ref[...] = hot_ref[...].T[0:64].astype(BF16)
        ranks = [rank_ref[c] for c in range(CELL)]

        @pl.when(jnp.logical_not(holder))
        def _():
            pltpu.make_async_copy(recv_d, recv_d, recv_sem.at[2]).wait()

        wait_rows(all_x, CELL - 1, recv_sem.at[3])

        grad_rows = []
        colours = []
        my_rank = rank_ref[cell]
        for h in range(HALVES):
            dense = recv_d[h]
            parts = [all_x[c, h] for c in range(CELL)]
            logs, dots = [], []
            for c in range(CELL):
                last = jnp.where(chan8 == 3, parts[c], 0.0)
                logs.append(last + pltpu.roll(last, 124, 1) + pltpu.roll(last, 120, 1) + pltpu.roll(last, 116, 1))
                lossy = parts[c] * dense
                dots.append(pltpu.roll(lossy, 4, 1) + pltpu.roll(lossy, 8, 1) + pltpu.roll(lossy, 12, 1))
            colour = jnp.zeros((8, GP), F32)
            behind = jnp.zeros((8, GP), F32)
            for c in range(CELL):
                shade = jnp.zeros((8, GP), F32)
                for other in range(CELL):
                    if other != c:
                        shade += jnp.where(ranks[other] < ranks[c], logs[other], 0.0)
                lit = jnp.exp(shade)
                lit_ref[h, c] = lit
                colour += lit * parts[c]
                behind += jnp.where(ranks[c] > my_rank, lit * dots[c], 0.0)
            colours.append(colour)
            d_part = dense * lit_ref[h, cell]
            of_half = [None] * LIST
            for entry in reversed(range(LIST)):
                d_c = dens_ref[h, entry] * d_part
                of_half[entry] = jnp.where(chan8 < 3, d_c, behind)
                lossy = d_c * entry_c[h, entry]
                behind = behind + (pltpu.roll(lossy, 4, 1) + pltpu.roll(lossy, 8, 1) + pltpu.roll(lossy, 12, 1))
            grad_rows += of_half
        pick = pick_ref[...]
        g_hi, g_lo = split(jnp.concatenate(grad_rows, axis=0))
        wide = mm(jnp.concatenate([g_hi, g_lo], axis=1), unfold_ref[...])
        columns = []
        for h in range(HALVES):
            spread = jnp.concatenate([wide[96 * h : 96 * h + 96, 128 * a : 128 * a + 128] for a in range(8)], axis=0)
            spread_hi, spread_lo = split(spread)
            columns += [spread_hi * pick, spread_lo * pick]
        back = mm(hot_t_ref[...], jnp.concatenate(columns, axis=1))
        for h in range(HALVES):
            send_f[pl.ds(h, 64, stride=2), :] = back[:, 256 * h : 256 * h + 128] + back[:, 256 * h + 128 : 256 * h + 256]
        far_first(
            lambda peer: pltpu.make_async_remote_copy(
                send_f.at[pl.ds(2 * peer, 2)], recv_f.at[pl.ds(2 * pair_of, 2)], send_sem.at[4], recv_sem.at[4],
                device_id=(cell, peer), device_id_type=MESH,
            ).start()
        )
        for i in range(HALVES):
            recv_f[pl.ds(2 * pair_of + i, 1), :] = send_f[pl.ds(2 * own + i, 1), :]

        @pl.when(holder)
        def _():
            for h in range(HALVES):
                for a in range(8):
                    send_c[pl.ds(16 * a + h, 8, stride=2), :] = pltpu.roll(colours[h], (GP - 16 * a) % GP, 1)
            far_first(
                lambda peer: pltpu.make_async_remote_copy(
                    send_c.at[pl.ds(2 * peer, 2)], recv_c.at[pl.ds(2 * own_z, 2)], send_sem.at[5], recv_sem.at[5],
                    device_id=(cell, peer), device_id_type=MESH,
                ).start()
            )
            for i in range(HALVES):
                recv_c[pl.ds(2 * own_z + i, 1), :] = send_c[pl.ds(2 * own + i, 1), :]

    @pl.when(head)
    def _():
        composite()

    after_of = (iota((2 * GP, GP), 0) % GP > iota((2 * GP, GP), 1)).astype(F32).astype(BF16)

    @pl.when(head)
    def _():
        wait_rows(recv_f, OWN - 2, recv_sem.at[4])

    @pl.when(not_head)
    def _():
        wait_rows(recv_f, OWN, recv_sem.at[4])

    cot = recv_f[...]
    cot_hi = cot.astype(BF16).astype(F32)
    cot_lo = cot - cot_hi
    lane64 = iota((64, GP), 1)
    left = []
    for r in range(NPX):
        one = pltpu.roll(cot_hi, (GP - 32 * r) % GP, 1)
        two = pltpu.roll(cot_hi, (GP + 32 - 32 * r) % GP, 1)
        three = pltpu.roll(cot_lo, (GP + 64 - 32 * r) % GP, 1)
        left.append(jnp.where(lane64 < 32, one, jnp.where(lane64 < 64, two, jnp.where(lane64 < 96, three, 0.0))))
    left = jnp.concatenate(left, axis=0).astype(BF16)
    turned = jnp.concatenate([cot, jnp.zeros((64, GP), F32)], axis=0).T
    turned = jnp.concatenate(
        [
            turned[0:32] + pltpu.roll(turned[32:64], 64, 1),
            turned[64:96] + pltpu.roll(turned[96:128], 64, 1),
        ],
        axis=1,
    )
    turned = jnp.concatenate(split(turned), axis=0)
    d_colour = jnp.zeros((32, GP), F32)
    for b in range(BLK):
        of = lambda v: jnp.broadcast_to(v[b : b + 1, :], (8, GP))
        mx, my = of(mean_x), of(mean_y)
        pair = mm(left, wcol_ref[b])
        d_before = pair[:, 0:128] * w_ref[b]
        after = mm(jnp.concatenate(split(d_before), axis=1), after_of)
        flow = (d_before - (pair[:, 128:256] + after) * u_ref[b]).reshape(NPX, 8, 8, GP)
        dy = ys - my[None]
        m0 = mxs = mxx = mys = mxy = myy = jnp.zeros((8, GP), F32)
        for r in range(NPX):
            dx = xs[r] - mx
            q = flow[r]
            qy = q * dy
            s0, s1 = jnp.sum(q, axis=0), jnp.sum(qy, axis=0)
            m0 += s0
            mxs += s0 * dx
            mxx += s0 * dx * dx
            mys += s1
            mxy += s1 * dx
            myy += jnp.sum(qy * dy, axis=0)
        for i, m in enumerate((m0, mxs, mxx, mys, mxy, myy)):
            mom_ref[i, b : b + 1, :] = jnp.sum(m, axis=0, keepdims=True)
        grown = mm(turned, wsplit_ref[b])
        grown = grown[0:32, 0:128] + grown[0:32, 128:256] + grown[32:64, 0:128]
        d_colour = jnp.where(row32 // 4 == b, grown, d_colour)
    m0, mxs, mxx, mys, mxy, myy = (mom_ref[i] for i in range(6))
    grad_ref[0] = inv_a * mxs + cross * mys
    grad_ref[1] = inv_c * mys + cross * mxs
    grad_ref[2] = -0.5 * (inv_a * mxx + cross * mxy)
    grad_ref[3] = -0.5 * (inv_c * myy + cross * mxy)
    grad_ref[4] = -mid * mxy
    grad_ref[5] = (1.0 - opacity) * m0
    crow_ref[...] = d_colour
    for k in range(3):
        grad_ref[6 + k] = crow_ref[pl.ds(k, 8, stride=4), :]

    @pl.when(holder)
    def _():
        wait_rows(recv_c, 6, recv_sem.at[5])

    @pl.when(jnp.logical_not(holder))
    def _():
        wait_rows(recv_c, 8, recv_sem.at[5])

    tile = pltpu.roll(recv_c[...], 0, 1, stride=4, stride_axis=0)
    for k in range(3):
        moved = pltpu.roll(tile, (GP - 4 * k) % GP, 1)
        moved = jnp.where(lane8 // 4 == row8, moved, 0.0)
        colour_ref[k] = jnp.sum(moved, axis=0, keepdims=True)[:, 0:32]

    @pl.when(head)
    def _():
        wait_rows(send_b, 3 * (HEADS - 1), send_sem.at[0])
        wait_rows(send_f, 2 * (OWN - 1), send_sem.at[4])
        wait_rows(all_x, CELL - 1, send_sem.at[3])

    @pl.when(not_head)
    def _():
        wait_rows(send_b, 3 * HEADS, send_sem.at[0])

    @pl.when(holder)
    def _():
        wait_rows(send_c, 2 * (OWN - 1), send_sem.at[5])
        wait_rows(all_x, CELL - 1, send_sem.at[2])


def put(colour_ref, grad_ref, colour_out, grad_out, sem):
    one = pltpu.make_async_copy(colour_ref, colour_out, sem.at[0])
    two = pltpu.make_async_copy(grad_ref, grad_out, sem.at[1])
    two.start()
    one.start()
    two.wait()
    one.wait()


def finish(colour, grads):
    vmem = pl.BlockSpec(memory_space=pltpu.VMEM)
    hbm = pl.BlockSpec(memory_space=pltpu.HBM)
    return pl.pallas_call(
        put,
        out_shape=(jax.ShapeDtypeStruct(colour.shape, F32), jax.ShapeDtypeStruct(grads.shape, F32)),
        in_specs=[vmem, vmem],
        out_specs=(hbm, hbm),
        scratch_shapes=[pltpu.SemaphoreType.DMA((2,))],
        compiler_params=pltpu.CompilerParams(vmem_limit_bytes=1 << 20),
    )(colour, grads)


def body(gaussians, fetch_ids, tile_lists, counts, cell_rank, d_colour):
    fetch = jnp.transpose(fetch_ids, (0, 1, 3, 2)).reshape(CAP, OWN)
    lists = tile_lists.reshape(1, LIST)
    hb = lambda v: pltpu.with_memory_space_constraint(v, pltpu.HBM)
    params = jnp.transpose(gaussians, (1, 0, 2))
    d_rows = jnp.transpose(d_colour, (1, 0, 2))
    hbm = pl.BlockSpec(memory_space=pltpu.HBM)
    vmem = pl.BlockSpec(memory_space=pltpu.VMEM)
    row = lambda n: pltpu.VMEM((n, GP), F32)
    colour, grads = pl.pallas_call(
        kernel,
        out_shape=(
            jax.ShapeDtypeStruct((3, 1, 32), F32),
            jax.ShapeDtypeStruct((9, BLK, GP), F32),
        ),
        in_specs=[hbm] * 6,
        out_specs=(vmem, vmem),
        scratch_shapes=[
            pltpu.SMEM((CAP, OWN), jnp.int32),
            pltpu.SMEM((1, LIST), jnp.int32),
            pltpu.SMEM((1, 1), jnp.int32),
            pltpu.SMEM((1, CELL), jnp.int32),
            pltpu.VMEM((9, BLK, GP), F32),
            pltpu.VMEM((3, 1, 32), F32),
            pltpu.SemaphoreType.DMA((6,)),
            pltpu.VMEM((BLK, 256, GP), F32),
            pltpu.VMEM((BLK, 256, GP), F32),
            pltpu.VMEM((BLK, 256, 256), BF16),
            pltpu.VMEM((BLK, GP, 256), BF16),
            pltpu.VMEM((32, GP), F32),
            pltpu.VMEM((6, 8, GP), F32),
            pltpu.VMEM((8, GP), F32),
            pltpu.VMEM((64, GP), F32),
            pltpu.VMEM((2048, 256), BF16),
            pltpu.VMEM((256, 1024), BF16),
            pltpu.VMEM((768, GP), F32),
            pltpu.VMEM((768, GP), BF16),
            pltpu.VMEM((64, 768), BF16),
            pltpu.VMEM((8, 8, GP), F32),
            pltpu.VMEM((HALVES, 8, 8, GP), F32),
            pltpu.VMEM((HALVES, LIST, 8, GP), F32),
            row(128), row(256),
            pltpu.VMEM((8, HALVES, 8, GP), F32),
            pltpu.VMEM((HALVES, 8, GP), F32),
            pltpu.VMEM((HALVES, 8, GP), F32),
            row(128), row(64), row(128), row(8),
            pltpu.SemaphoreType.DMA((6,)),
            pltpu.SemaphoreType.DMA((6,)),
        ],
        compiler_params=pltpu.CompilerParams(
            collective_id=0, has_side_effects=True, vmem_limit_bytes=32 << 20
        ),
    )(hb(fetch), hb(lists), counts, hb(cell_rank), hb(params), hb(d_rows))
    colour, grads = finish(colour, grads)
    return jnp.transpose(colour, (1, 0, 2)), jnp.transpose(grads, (1, 0, 2))


def solution(mesh):
    in_specs = (
        P(("cell", "own"), None, None),
        P("cell", "own", None, None),
        P("cell", "own", None),
        P("cell", "own"),
        P("own", None),
        P("own", None, "cell"),
    )
    out_specs = (P("own", None, "cell"), P(("cell", "own"), None, None))
    return jax.shard_map(body, mesh=mesh, in_specs=in_specs, out_specs=out_specs, check_vma=False)
```

```python
import jax
import jax.numpy as jnp
from jax import lax
from jax.experimental import pallas as pl
from jax.experimental.pallas import tpu as pltpu
from jax.sharding import PartitionSpec as P

MESH = pl.DeviceIdType.MESH
F32 = jnp.float32
BF16 = jnp.bfloat16

LIST = 12
CAP = 4
OWN = 64
CELL = 8
CELL_ORDER = (4, 3, 5, 2, 6, 1, 7)
BLK = 8
GP = 128
NPX = 4
HEADS = 32
HALVES = 2
LOG2E = 1.4426950408889634
L_PEER, L_RANK, L_BLK, L_DCOL = 0, 16, 32, 64


def iota(shape, dim):
    return lax.broadcasted_iota(jnp.int32, shape, dim)


def split(x):
    hi = x.astype(BF16)
    return hi, (x - hi.astype(F32)).astype(BF16)


def mm(a, b):
    return lax.dot_general(a, b, (((1,), (0,)), ((), ())), preferred_element_type=F32)


def mm_nt(a, b):
    return lax.dot_general(a, b, (((1,), (1,)), ((), ())), preferred_element_type=F32)


def wait_rows(ref, rows, sem):
    view = ref.at[pl.ds(0, rows)]
    pltpu.make_async_copy(view, view, sem).wait()


def kernel(
    fetch_h, list_h, count_h, rank_h, g_h, dcol_h,
    colour_ref, grad_ref,
    fetch_s, list_s, count_s, rank_s, g_ref, dcol_ref, in_sem,
    w_ref, u_ref, wsplit_ref, wcol_ref, crow_ref, mom_ref, dpad_ref, rows_ref,
    fold_ref, unfold_ref, hot_ref, pick_ref, hot_t_ref, rank_ref, lit_ref, dens_ref,
    send_b, recv_b, all_x, send_d, recv_d, send_f, recv_f, send_c, recv_c,
    send_sem, recv_sem,
):
    cell = lax.axis_index("cell")
    own = lax.axis_index("own")
    own_y = lax.div(own, 8)
    own_z = lax.rem(own, 8)
    moved_in = (own_y == 0) & (own_z >= 4)
    moved_out = (own_z == 3) & (own_y >= 3) & (own_y <= 6)
    head = (own_z < 4) & jnp.logical_not(moved_out) | moved_in
    not_head = jnp.logical_not(head)
    pair_y = jnp.where(moved_in, own_z - 1, own_y)
    pair_z = jnp.where(moved_in, 3, lax.rem(own_z, 4))
    pair_of = 4 * pair_y + pair_z
    holder = head & (pair_y == cell)

    def far_first(visit):
        def pair(k, carry):
            visit(lax.rem(own + 36 + k, OWN))
            visit(lax.rem(own + 35 - k, OWN))
            return carry

        def near(k, carry):
            visit(lax.rem(own + 7 - k, OWN))
            return carry

        lax.fori_loop(0, 28, pair, 0)
        lax.fori_loop(0, 7, near, 0)

    def early_first(visit):
        def one(k, carry):
            peer = 8 * lax.rem(own_y + 4 + lax.rem(k, 8), 8) + lax.div(k, 8)

            @pl.when(peer != own)
            def _():
                visit(peer)

            return carry

        lax.fori_loop(0, OWN, one, 0)

    barrier = pltpu.get_barrier_semaphore()

    @pl.when(head)
    def _():
        far_first(lambda peer: pl.semaphore_signal(barrier, inc=1, device_id=(cell, peer), device_id_type=MESH))
        for i in CELL_ORDER:
            pl.semaphore_signal(barrier, inc=1, device_id=(lax.rem(cell + i, CELL), own), device_id_type=MESH)

    loads = [
        pltpu.make_async_copy(source, target, in_sem.at[i])
        for i, (source, target) in enumerate(
            [(g_h, g_ref), (fetch_h, fetch_s), (list_h, list_s), (count_h, count_s), (rank_h, rank_s), (dcol_h, dcol_ref)]
        )
    ]
    for load in loads:
        load.start()

    lane1 = iota((1, GP), 1)
    lane8 = iota((8, GP), 1)
    row8 = iota((8, GP), 0)
    chan8 = (lane8 % 16) // 4

    for load in loads:
        load.wait()
    live_n = count_s[0, 0]
    aux = jnp.zeros((1, GP), jnp.int32)
    for entry in range(LIST):
        slot = list_s[0, entry]
        peer = slot // CAP
        block = fetch_s[slot % CAP, peer] - peer * BLK
        live = (entry < live_n).astype(jnp.int32)
        aux = jnp.where(lane1 == L_PEER + entry, live * (peer + 1) - 1, aux)
        aux = jnp.where(lane1 == L_BLK + entry, block, aux)
    for c in range(CELL):
        aux = jnp.where(lane1 == L_RANK + c, rank_s[0, c], aux)
    aux = jnp.broadcast_to(aux.astype(F32), (8, GP))
    dpad_ref[...] = jnp.zeros((8, GP), F32)
    for k in range(3):
        dpad_ref[k : k + 1, 0:32] = dcol_ref[k]
    slanted = pltpu.roll(dpad_ref[...], 0, 1, stride=4, stride_axis=0)
    of_row = ((lane8 - L_DCOL) // 4 == row8) & (lane8 >= L_DCOL) & (row8 < 3)
    dcol_rows = jnp.zeros((8, GP), F32)
    for i in range(8):
        moved = jnp.where(of_row, pltpu.roll(slanted, L_DCOL - 4 * i, 1), 0.0)
        moved = jnp.broadcast_to(jnp.sum(moved, axis=0, keepdims=True), (8, GP))
        dcol_rows = jnp.where(row8 == i, moved, dcol_rows)
    rows_ref[0:8, :] = dcol_rows
    two_groups = rows_ref[pl.ds(0, 4, stride=2), :] + pltpu.roll(rows_ref[pl.ds(1, 4, stride=2), :], 16, 1)
    for i in range(8):
        mine = (cell == i).astype(F32)
        send_b[pl.ds(16 * i + 2, 4, stride=4), :] = aux[0:4] + mine * two_groups

    mean_x, mean_y = g_ref[0], g_ref[1]
    inv_a, inv_c = jnp.exp(g_ref[2]), jnp.exp(g_ref[3])
    mid = jnp.exp(0.5 * (g_ref[2] + g_ref[3]))
    cross = g_ref[4] * mid
    opacity = jax.nn.sigmoid(g_ref[5])
    crow_ref[...] = jnp.zeros((32, GP), F32)
    for k in range(3):
        crow_ref[pl.ds(k, 8, stride=4), :] = g_ref[6 + k]
    crow = crow_ref[...]
    row32 = iota((32, GP), 0)
    before_of = (iota((2 * GP, 2 * GP), 0) % GP < iota((2 * GP, 2 * GP), 1)).astype(F32).astype(BF16)
    log_op = LOG2E * jnp.log(opacity)
    half_a, half_c, cross2 = (0.5 * LOG2E) * inv_a, (0.5 * LOG2E) * inv_c, LOG2E * cross
    xs = [(4 * (row8 % 4) + r).astype(F32) + 0.5 for r in range(NPX)]
    ys = (2 * iota((8, 8, GP), 0) + iota((8, 8, GP), 1) // 4).astype(F32) + 0.5

    lane256 = iota((256, GP), 1)
    total = jnp.zeros((256, 64), F32)
    logs = jnp.zeros((256, GP), F32)
    for b in range(BLK):
        of = lambda v: jnp.broadcast_to(v[b : b + 1, :], (8, GP))
        mx, my, ca, cc, cb, op = (of(v) for v in (mean_x, mean_y, half_a, half_c, cross2, log_op))
        dy = ys - my[None]
        part_y = op[None] - cc[None] * dy * dy
        slope = cb[None] * dy
        covs = []
        for r in range(NPX):
            dx = xs[r] - mx
            covs.append(jnp.exp2(part_y - (ca * dx * dx)[None] - dx[None] * slope))
        cov = jnp.stack(covs, axis=0).reshape(256, GP)
        before = mm(jnp.concatenate(split(jnp.log(1.0 - cov)), axis=1), before_of)
        weight = jnp.exp(before[:, 0:GP]) * cov
        logs = jnp.where(lane256 == 4 * b + 3, before[:, GP:], logs)
        c_hi, c_lo = split(jnp.where(row32 // 4 == b, crow, 0.0))
        both = jnp.concatenate(
            [jnp.concatenate([c_hi, c_hi], axis=1), jnp.concatenate([c_lo, jnp.zeros((32, GP), BF16)], axis=1)], axis=0
        )
        total += mm_nt(jnp.concatenate(split(weight), axis=1), both)
        w_ref[b] = weight
        u_ref[b] = cov
    total = jnp.concatenate([total, jnp.zeros((256, 64), F32)], axis=1)
    total = jnp.where(lane256 < 32, total + pltpu.roll(total, 96, 1) + logs, 0.0)
    rows = total[0:64]
    for r in range(1, NPX):
        rows += pltpu.roll(total[64 * r : 64 * r + 64], 32 * r, 1)
    rows_ref[...] = rows
    for h in range(HALVES):
        send_b[pl.ds(h, HEADS, stride=4), :] = rows_ref[pl.ds(h, HEADS, stride=2), :]

    pl.semaphore_wait(barrier, jnp.where(head, HEADS - 1 + CELL - 1, HEADS))

    def to_head(pair):
        row = lax.div(pair, 4)
        late = (lax.rem(pair, 4) == 3) & (row >= 3) & (row <= 6)
        peer = jnp.where(late, row + 1, pair + 4 * row)

        @pl.when(peer != own)
        def _():
            pltpu.make_async_remote_copy(
                send_b.at[pl.ds(4 * pair, 3)], recv_b.at[pl.ds(4 * own, 3)], send_sem.at[0], recv_sem.at[0],
                device_id=(cell, peer), device_id_type=MESH,
            ).start()

    def to_two_heads(k, carry):
        to_head(lax.rem(4 * own_y + 16 + k, HEADS))
        to_head(lax.rem(4 * own_y + 47 - k, HEADS))
        return carry

    lax.fori_loop(0, HEADS // 2, to_two_heads, 0)

    for b in range(BLK):
        cov = u_ref[b]
        u_ref[b] = cov / (1.0 - cov)
        wsplit_ref[b] = jnp.concatenate(split(w_ref[b]), axis=1)
        ones_b = jnp.where(row32 == 4 * b + 3, 1.0, 0.0).astype(BF16)
        c_hi, c_lo = split(jnp.where(row32 // 4 == b, crow, 0.0))
        none = jnp.zeros((32, GP), BF16)
        top = jnp.concatenate([c_hi, ones_b], axis=1)
        low = jnp.concatenate([c_lo, none], axis=1)
        wcol_ref[b] = jnp.concatenate([top, low, top, jnp.concatenate([none, none], axis=1)], axis=0)

    def composite():
        for a in range(8):
            lane_in = iota((GP, GP), 0)
            lane_out = iota((GP, GP), 1)
            same = (lane_out // 16 == a) & (lane_out % 4 == lane_in // 32)
            to_own = same & ((lane_out % 16) // 4 == lane_in % 4)
            to_all = same & (lane_in % 4 == 3)
            piece = jnp.concatenate([to_own.astype(F32), to_all.astype(F32)], axis=1).astype(BF16)
            fold_ref[256 * a : 256 * a + 128, :] = piece
            fold_ref[256 * a + 128 : 256 * a + 256, :] = piece
            back = (lane_in // 16 == a) & (lane_in % 4 == lane_out // 32) & ((lane_in % 16) // 4 == lane_out % 4)
            back = back.astype(F32).astype(BF16)
            unfold_ref[0:128, 128 * a : 128 * a + 128] = back
            unfold_ref[128:256, 128 * a : 128 * a + 128] = back

        choose_in = iota((GP, 256), 0)
        choose_out = iota((GP, 256), 1)
        choose = (choose_in < 16) & (choose_out < 128) | (choose_in >= 32) & (choose_in < 48) & (choose_out >= 128)
        choose = choose.astype(F32).astype(BF16)
        for i in range(3):
            recv_b[pl.ds(4 * own + i, 1), :] = send_b[pl.ds(4 * pair_of + i, 1), :]
        wait_rows(recv_b, 3 * (OWN - 1), recv_sem.at[0])
        lane8f = lane8.astype(F32)
        block8f = ((lane8 // 4) % 8).astype(F32)
        dense_d = [jnp.zeros((8, GP), F32)] * HALVES
        dense_r = jnp.zeros((8, GP), F32)
        lone = []
        for a in range(8):
            tile_rows = recv_b[pl.ds(32 * a + 2, 8, stride=4), :]
            here = lane8 // 16 == a
            dense_d = [
                jnp.where(here, pltpu.roll(tile_rows, (16 * a - L_DCOL - 16 * h) % GP, 1), dense_d[h]) for h in range(HALVES)
            ]
            dense_r = jnp.where(here, pltpu.roll(tile_rows, (16 * a - L_RANK) % GP, 1), dense_r)
            for entry in range(LIST):
                mine = (lane8 == L_PEER + entry) | (lane8 == L_BLK + entry)
                lone.append(jnp.where(mine, tile_rows, 0.0))
        named = mm(jnp.concatenate(lone, axis=0).astype(BF16), choose).reshape(96, 8, 256)
        hot = jnp.where(named[:, :, 0:128] == lane8f[None], 1.0, 0.0).reshape(768, GP)
        pick = jnp.where(named[:, :, 128:256] == block8f[None], 1.0, 0.0).reshape(768, GP).astype(BF16)
        hot_ref[...] = hot
        pick_ref[...] = pick
        dense_d = [jnp.where(chan8 < 3, dense_d[h], 0.0) for h in range(HALVES)]

        @pl.when(holder)
        def _():
            for h in range(HALVES):
                send_d[h] = dense_d[h]
                recv_d[h] = dense_d[h]
            for i in CELL_ORDER:
                pltpu.make_async_remote_copy(
                    send_d, recv_d, send_sem.at[2], recv_sem.at[2],
                    device_id=(lax.rem(cell + i, CELL), own), device_id_type=MESH,
                ).start()

        one_rank = jnp.concatenate([jnp.where(lane8 % 16 == c, dense_r, 0.0) for c in range(CELL)], axis=0)
        group = (iota((GP, GP), 0) // 16 == iota((GP, GP), 1) // 16).astype(F32).astype(BF16)
        rank_ref[...] = mm(one_rank.astype(BF16), group).reshape(8, 8, GP)

        pieces = []
        for h in range(HALVES):
            pieces += split(recv_b[pl.ds(h, 64, stride=4), :])
        taken = mm(hot.astype(BF16)[:, 0:64], jnp.concatenate(pieces, axis=1)).astype(BF16)
        taken = taken * jnp.concatenate([pick] * 4, axis=1)
        taken = jnp.concatenate(
            [
                jnp.concatenate([taken[96 * a : 96 * a + 96, 256 * h : 256 * h + 256] for a in range(8)], axis=1)
                for h in range(HALVES)
            ],
            axis=0,
        )
        folded = mm(taken, fold_ref[...])
        entry_c = folded[:, 0:128].reshape(HALVES, LIST, 8, GP)
        entry_t = folded[:, 128:256].reshape(HALVES, LIST, 8, GP)
        for h in range(HALVES):
            ahead = jnp.zeros((8, GP), F32)
            part = jnp.zeros((8, GP), F32)
            for entry in range(LIST):
                seen = jnp.exp(ahead)
                dens_ref[h, entry] = seen
                part += seen * entry_c[h, entry]
                ahead += entry_t[h, entry]
            all_x[cell, h] = jnp.where(chan8 < 3, part, ahead)
        for i in CELL_ORDER:
            pltpu.make_async_remote_copy(
                all_x.at[cell], all_x.at[cell], send_sem.at[3], recv_sem.at[3],
                device_id=(lax.rem(cell + i, CELL), own), device_id_type=MESH,
            ).start()

        hot_t_ref[...] = hot_ref[...].T[0:64].astype(BF16)
        ranks = [rank_ref[c] for c in range(CELL)]

        @pl.when(jnp.logical_not(holder))
        def _():
            pltpu.make_async_copy(recv_d, recv_d, recv_sem.at[2]).wait()

        wait_rows(all_x, CELL - 1, recv_sem.at[3])

        grad_rows = []
        colours = []
        my_rank = rank_ref[cell]
        for h in range(HALVES):
            dense = recv_d[h]
            parts = [all_x[c, h] for c in range(CELL)]
            logs, dots = [], []
            for c in range(CELL):
                last = jnp.where(chan8 == 3, parts[c], 0.0)
                logs.append(last + pltpu.roll(last, 124, 1) + pltpu.roll(last, 120, 1) + pltpu.roll(last, 116, 1))
                lossy = parts[c] * dense
                dots.append(pltpu.roll(lossy, 4, 1) + pltpu.roll(lossy, 8, 1) + pltpu.roll(lossy, 12, 1))
            colour = jnp.zeros((8, GP), F32)
            behind = jnp.zeros((8, GP), F32)
            for c in range(CELL):
                shade = jnp.zeros((8, GP), F32)
                for other in range(CELL):
                    if other != c:
                        shade += jnp.where(ranks[other] < ranks[c], logs[other], 0.0)
                lit = jnp.exp(shade)
                lit_ref[h, c] = lit
                colour += lit * parts[c]
                behind += jnp.where(ranks[c] > my_rank, lit * dots[c], 0.0)
            colours.append(colour)
            d_part = dense * lit_ref[h, cell]
            of_half = [None] * LIST
            for entry in reversed(range(LIST)):
                d_c = dens_ref[h, entry] * d_part
                of_half[entry] = jnp.where(chan8 < 3, d_c, behind)
                lossy = d_c * entry_c[h, entry]
                behind = behind + (pltpu.roll(lossy, 4, 1) + pltpu.roll(lossy, 8, 1) + pltpu.roll(lossy, 12, 1))
            grad_rows += of_half
        pick = pick_ref[...]
        g_hi, g_lo = split(jnp.concatenate(grad_rows, axis=0))
        wide = mm(jnp.concatenate([g_hi, g_lo], axis=1), unfold_ref[...])
        columns = []
        for h in range(HALVES):
            spread = jnp.concatenate([wide[96 * h : 96 * h + 96, 128 * a : 128 * a + 128] for a in range(8)], axis=0)
            spread_hi, spread_lo = split(spread)
            columns += [spread_hi * pick, spread_lo * pick]
        back = mm(hot_t_ref[...], jnp.concatenate(columns, axis=1))
        for h in range(HALVES):
            send_f[pl.ds(h, 64, stride=2), :] = back[:, 256 * h : 256 * h + 128] + back[:, 256 * h + 128 : 256 * h + 256]
        early_first(
            lambda peer: pltpu.make_async_remote_copy(
                send_f.at[pl.ds(2 * peer, 2)], recv_f.at[pl.ds(2 * pair_of, 2)], send_sem.at[4], recv_sem.at[4],
                device_id=(cell, peer), device_id_type=MESH,
            ).start()
        )
        for i in range(HALVES):
            recv_f[pl.ds(2 * pair_of + i, 1), :] = send_f[pl.ds(2 * own + i, 1), :]

        @pl.when(holder)
        def _():
            for h in range(HALVES):
                for a in range(8):
                    send_c[pl.ds(16 * a + h, 8, stride=2), :] = pltpu.roll(colours[h], (GP - 16 * a) % GP, 1)
            far_first(
                lambda peer: pltpu.make_async_remote_copy(
                    send_c.at[pl.ds(2 * peer, 2)], recv_c.at[pl.ds(2 * pair_z, 2)], send_sem.at[5], recv_sem.at[5],
                    device_id=(cell, peer), device_id_type=MESH,
                ).start()
            )
            for i in range(HALVES):
                recv_c[pl.ds(2 * pair_z + i, 1), :] = send_c[pl.ds(2 * own + i, 1), :]

    @pl.when(head)
    def _():
        composite()

    after_of = (iota((2 * GP, GP), 0) % GP > iota((2 * GP, GP), 1)).astype(F32).astype(BF16)

    @pl.when(head)
    def _():
        wait_rows(recv_f, OWN - 2, recv_sem.at[4])

    @pl.when(not_head)
    def _():
        wait_rows(recv_f, OWN, recv_sem.at[4])

    cot = recv_f[...]
    cot_hi = cot.astype(BF16).astype(F32)
    cot_lo = cot - cot_hi
    lane64 = iota((64, GP), 1)
    left = []
    for r in range(NPX):
        one = pltpu.roll(cot_hi, (GP - 32 * r) % GP, 1)
        two = pltpu.roll(cot_hi, (GP + 32 - 32 * r) % GP, 1)
        three = pltpu.roll(cot_lo, (GP + 64 - 32 * r) % GP, 1)
        left.append(jnp.where(lane64 < 32, one, jnp.where(lane64 < 64, two, jnp.where(lane64 < 96, three, 0.0))))
    left = jnp.concatenate(left, axis=0).astype(BF16)
    turned = jnp.concatenate([cot, jnp.zeros((64, GP), F32)], axis=0).T
    turned = jnp.concatenate(
        [
            turned[0:32] + pltpu.roll(turned[32:64], 64, 1),
            turned[64:96] + pltpu.roll(turned[96:128], 64, 1),
        ],
        axis=1,
    )
    turned = jnp.concatenate(split(turned), axis=0)
    d_colour = jnp.zeros((32, GP), F32)
    for b in range(BLK):
        of = lambda v: jnp.broadcast_to(v[b : b + 1, :], (8, GP))
        mx, my = of(mean_x), of(mean_y)
        pair = mm(left, wcol_ref[b])
        d_before = pair[:, 0:128] * w_ref[b]
        after = mm(jnp.concatenate(split(d_before), axis=1), after_of)
        flow = (d_before - (pair[:, 128:256] + after) * u_ref[b]).reshape(NPX, 8, 8, GP)
        dy = ys - my[None]
        m0 = mxs = mxx = mys = mxy = myy = jnp.zeros((8, GP), F32)
        for r in range(NPX):
            dx = xs[r] - mx
            q = flow[r]
            qy = q * dy
            s0, s1 = jnp.sum(q, axis=0), jnp.sum(qy, axis=0)
            m0 += s0
            mxs += s0 * dx
            mxx += s0 * dx * dx
            mys += s1
            mxy += s1 * dx
            myy += jnp.sum(qy * dy, axis=0)
        for i, m in enumerate((m0, mxs, mxx, mys, mxy, myy)):
            mom_ref[i, b : b + 1, :] = jnp.sum(m, axis=0, keepdims=True)
        grown = mm(turned, wsplit_ref[b])
        grown = grown[0:32, 0:128] + grown[0:32, 128:256] + grown[32:64, 0:128]
        d_colour = jnp.where(row32 // 4 == b, grown, d_colour)
    m0, mxs, mxx, mys, mxy, myy = (mom_ref[i] for i in range(6))
    grad_ref[0] = inv_a * mxs + cross * mys
    grad_ref[1] = inv_c * mys + cross * mxs
    grad_ref[2] = -0.5 * (inv_a * mxx + cross * mxy)
    grad_ref[3] = -0.5 * (inv_c * myy + cross * mxy)
    grad_ref[4] = -mid * mxy
    grad_ref[5] = (1.0 - opacity) * m0
    crow_ref[...] = d_colour
    for k in range(3):
        grad_ref[6 + k] = crow_ref[pl.ds(k, 8, stride=4), :]

    @pl.when(holder)
    def _():
        wait_rows(recv_c, 6, recv_sem.at[5])

    @pl.when(jnp.logical_not(holder))
    def _():
        wait_rows(recv_c, 8, recv_sem.at[5])

    tile = pltpu.roll(recv_c[...], 0, 1, stride=4, stride_axis=0)
    for k in range(3):
        moved = pltpu.roll(tile, (GP - 4 * k) % GP, 1)
        moved = jnp.where(lane8 // 4 == row8, moved, 0.0)
        colour_ref[k] = jnp.sum(moved, axis=0, keepdims=True)[:, 0:32]

    @pl.when(head)
    def _():
        wait_rows(send_b, 3 * (HEADS - 1), send_sem.at[0])
        wait_rows(send_f, 2 * (OWN - 1), send_sem.at[4])
        wait_rows(all_x, CELL - 1, send_sem.at[3])

    @pl.when(not_head)
    def _():
        wait_rows(send_b, 3 * HEADS, send_sem.at[0])

    @pl.when(holder)
    def _():
        wait_rows(send_c, 2 * (OWN - 1), send_sem.at[5])
        wait_rows(all_x, CELL - 1, send_sem.at[2])


def put(colour_ref, grad_ref, colour_out, grad_out, sem):
    one = pltpu.make_async_copy(colour_ref, colour_out, sem.at[0])
    two = pltpu.make_async_copy(grad_ref, grad_out, sem.at[1])
    two.start()
    one.start()
    two.wait()
    one.wait()


def finish(colour, grads):
    vmem = pl.BlockSpec(memory_space=pltpu.VMEM)
    hbm = pl.BlockSpec(memory_space=pltpu.HBM)
    return pl.pallas_call(
        put,
        out_shape=(jax.ShapeDtypeStruct(colour.shape, F32), jax.ShapeDtypeStruct(grads.shape, F32)),
        in_specs=[vmem, vmem],
        out_specs=(hbm, hbm),
        scratch_shapes=[pltpu.SemaphoreType.DMA((2,))],
        compiler_params=pltpu.CompilerParams(vmem_limit_bytes=1 << 20),
    )(colour, grads)


def body(gaussians, fetch_ids, tile_lists, counts, cell_rank, d_colour):
    fetch = jnp.transpose(fetch_ids, (0, 1, 3, 2)).reshape(CAP, OWN)
    lists = tile_lists.reshape(1, LIST)
    hb = lambda v: pltpu.with_memory_space_constraint(v, pltpu.HBM)
    params = jnp.transpose(gaussians, (1, 0, 2))
    d_rows = jnp.transpose(d_colour, (1, 0, 2))
    hbm = pl.BlockSpec(memory_space=pltpu.HBM)
    vmem = pl.BlockSpec(memory_space=pltpu.VMEM)
    row = lambda n: pltpu.VMEM((n, GP), F32)
    colour, grads = pl.pallas_call(
        kernel,
        out_shape=(
            jax.ShapeDtypeStruct((3, 1, 32), F32),
            jax.ShapeDtypeStruct((9, BLK, GP), F32),
        ),
        in_specs=[hbm] * 6,
        out_specs=(vmem, vmem),
        scratch_shapes=[
            pltpu.SMEM((CAP, OWN), jnp.int32),
            pltpu.SMEM((1, LIST), jnp.int32),
            pltpu.SMEM((1, 1), jnp.int32),
            pltpu.SMEM((1, CELL), jnp.int32),
            pltpu.VMEM((9, BLK, GP), F32),
            pltpu.VMEM((3, 1, 32), F32),
            pltpu.SemaphoreType.DMA((6,)),
            pltpu.VMEM((BLK, 256, GP), F32),
            pltpu.VMEM((BLK, 256, GP), F32),
            pltpu.VMEM((BLK, 256, 256), BF16),
            pltpu.VMEM((BLK, GP, 256), BF16),
            pltpu.VMEM((32, GP), F32),
            pltpu.VMEM((6, 8, GP), F32),
            pltpu.VMEM((8, GP), F32),
            pltpu.VMEM((64, GP), F32),
            pltpu.VMEM((2048, 256), BF16),
            pltpu.VMEM((256, 1024), BF16),
            pltpu.VMEM((768, GP), F32),
            pltpu.VMEM((768, GP), BF16),
            pltpu.VMEM((64, 768), BF16),
            pltpu.VMEM((8, 8, GP), F32),
            pltpu.VMEM((HALVES, 8, 8, GP), F32),
            pltpu.VMEM((HALVES, LIST, 8, GP), F32),
            row(128), row(256),
            pltpu.VMEM((8, HALVES, 8, GP), F32),
            pltpu.VMEM((HALVES, 8, GP), F32),
            pltpu.VMEM((HALVES, 8, GP), F32),
            row(128), row(64), row(128), row(8),
            pltpu.SemaphoreType.DMA((6,)),
            pltpu.SemaphoreType.DMA((6,)),
        ],
        compiler_params=pltpu.CompilerParams(
            collective_id=0, has_side_effects=True, vmem_limit_bytes=32 << 20
        ),
    )(hb(fetch), hb(lists), counts, hb(cell_rank), hb(params), hb(d_rows))
    colour, grads = finish(colour, grads)
    return jnp.transpose(colour, (1, 0, 2)), jnp.transpose(grads, (1, 0, 2))


def solution(mesh):
    in_specs = (
        P(("cell", "own"), None, None),
        P("cell", "own", None, None),
        P("cell", "own", None),
        P("cell", "own"),
        P("own", None),
        P("own", None, "cell"),
    )
    out_specs = (P("own", None, "cell"), P(("cell", "own"), None, None))
    return jax.shard_map(body, mesh=mesh, in_specs=in_specs, out_specs=out_specs, check_vma=False)
```

```python
import jax
import jax.numpy as jnp
from jax import lax
from jax.experimental import pallas as pl
from jax.experimental.pallas import tpu as pltpu
from jax.sharding import PartitionSpec as P

MESH = pl.DeviceIdType.MESH
F32 = jnp.float32
BF16 = jnp.bfloat16

LIST = 12
CAP = 4
OWN = 64
CELL = 8
CELL_ORDER = (4, 3, 5, 2, 6, 1, 7)
BLK = 8
GP = 128
NPX = 4
HEADS = 32
HALVES = 2
LOG2E = 1.4426950408889634
L_PEER, L_RANK, L_BLK, L_DCOL = 0, 16, 32, 64


def iota(shape, dim):
    return lax.broadcasted_iota(jnp.int32, shape, dim)


def split(x):
    hi = x.astype(BF16)
    return hi, (x - hi.astype(F32)).astype(BF16)


def mm(a, b):
    return lax.dot_general(a, b, (((1,), (0,)), ((), ())), preferred_element_type=F32)


def mm_nt(a, b):
    return lax.dot_general(a, b, (((1,), (1,)), ((), ())), preferred_element_type=F32)


def wait_rows(ref, rows, sem):
    view = ref.at[pl.ds(0, rows)]
    pltpu.make_async_copy(view, view, sem).wait()


def kernel(
    fetch_h, list_h, count_h, rank_h, g_h, dcol_h,
    colour_ref, grad_ref,
    fetch_s, list_s, count_s, rank_s, g_ref, dcol_ref, in_sem,
    w_ref, u_ref, wsplit_ref, wcol_ref, crow_ref, mom_ref, dpad_ref, rows_ref,
    fold_ref, unfold_ref, hot_ref, pick_ref, hot_t_ref, rank_ref, lit_ref, dens_ref,
    send_b, recv_b, all_x, send_d, recv_d, send_f, recv_f, send_c, recv_c,
    send_sem, recv_sem,
):
    cell = lax.axis_index("cell")
    own = lax.axis_index("own")
    own_y = lax.div(own, 8)
    own_z = lax.rem(own, 8)
    moved_in = (own_y == 0) & (own_z >= 4)
    moved_out = (own_z == 3) & (own_y >= 3) & (own_y <= 6)
    head = (own_z < 4) & jnp.logical_not(moved_out) | moved_in
    not_head = jnp.logical_not(head)
    pair_y = jnp.where(moved_in, own_z - 1, own_y)
    pair_z = jnp.where(moved_in, 3, lax.rem(own_z, 4))
    pair_of = 4 * pair_y + pair_z
    holder = head & (pair_y == cell)

    def far_first(visit):
        def pair(k, carry):
            visit(lax.rem(own + 36 + k, OWN))
            visit(lax.rem(own + 35 - k, OWN))
            return carry

        def near(k, carry):
            visit(lax.rem(own + 7 - k, OWN))
            return carry

        lax.fori_loop(0, 28, pair, 0)
        lax.fori_loop(0, 7, near, 0)

    def early_first(visit):
        def one(k, carry):
            peer = 8 * lax.rem(own_y + 4 + lax.rem(k, 8), 8) + lax.div(k, 8)

            @pl.when(peer != own)
            def _():
                visit(peer)

            return carry

        lax.fori_loop(0, OWN, one, 0)

    barrier = pltpu.get_barrier_semaphore()

    @pl.when(head)
    def _():
        far_first(lambda peer: pl.semaphore_signal(barrier, inc=1, device_id=(cell, peer), device_id_type=MESH))
        for i in CELL_ORDER:
            pl.semaphore_signal(barrier, inc=1, device_id=(lax.rem(cell + i, CELL), own), device_id_type=MESH)

    loads = [
        pltpu.make_async_copy(source, target, in_sem.at[i])
        for i, (source, target) in enumerate(
            [(g_h, g_ref), (fetch_h, fetch_s), (list_h, list_s), (count_h, count_s), (rank_h, rank_s), (dcol_h, dcol_ref)]
        )
    ]
    for load in loads:
        load.start()

    lane1 = iota((1, GP), 1)
    lane8 = iota((8, GP), 1)
    row8 = iota((8, GP), 0)
    chan8 = (lane8 % 16) // 4

    for load in loads:
        load.wait()
    live_n = count_s[0, 0]
    aux = jnp.zeros((1, GP), jnp.int32)
    for entry in range(LIST):
        slot = list_s[0, entry]
        peer = slot // CAP
        block = fetch_s[slot % CAP, peer] - peer * BLK
        live = (entry < live_n).astype(jnp.int32)
        aux = jnp.where(lane1 == L_PEER + entry, live * (peer + 1) - 1, aux)
        aux = jnp.where(lane1 == L_BLK + entry, block, aux)
    for c in range(CELL):
        aux = jnp.where(lane1 == L_RANK + c, rank_s[0, c], aux)
    aux = jnp.broadcast_to(aux.astype(F32), (8, GP))
    dpad_ref[...] = jnp.zeros((8, GP), F32)
    for k in range(3):
        dpad_ref[k : k + 1, 0:32] = dcol_ref[k]
    slanted = pltpu.roll(dpad_ref[...], 0, 1, stride=4, stride_axis=0)
    of_row = ((lane8 - L_DCOL) // 4 == row8) & (lane8 >= L_DCOL) & (row8 < 3)
    dcol_rows = jnp.zeros((8, GP), F32)
    for i in range(8):
        moved = jnp.where(of_row, pltpu.roll(slanted, L_DCOL - 4 * i, 1), 0.0)
        moved = jnp.broadcast_to(jnp.sum(moved, axis=0, keepdims=True), (8, GP))
        dcol_rows = jnp.where(row8 == i, moved, dcol_rows)
    rows_ref[0:8, :] = dcol_rows
    two_groups = rows_ref[pl.ds(0, 4, stride=2), :] + pltpu.roll(rows_ref[pl.ds(1, 4, stride=2), :], 16, 1)
    for i in range(8):
        mine = (cell == i).astype(F32)
        send_b[pl.ds(16 * i + 2, 4, stride=4), :] = aux[0:4] + mine * two_groups

    mean_x, mean_y = g_ref[0], g_ref[1]
    inv_a, inv_c = jnp.exp(g_ref[2]), jnp.exp(g_ref[3])
    mid = jnp.exp(0.5 * (g_ref[2] + g_ref[3]))
    cross = g_ref[4] * mid
    opacity = jax.nn.sigmoid(g_ref[5])
    crow_ref[...] = jnp.zeros((32, GP), F32)
    for k in range(3):
        crow_ref[pl.ds(k, 8, stride=4), :] = g_ref[6 + k]
    crow = crow_ref[...]
    row32 = iota((32, GP), 0)
    before_of = (iota((2 * GP, 2 * GP), 0) % GP < iota((2 * GP, 2 * GP), 1)).astype(F32).astype(BF16)
    log_op = LOG2E * jnp.log(opacity)
    half_a, half_c, cross2 = (0.5 * LOG2E) * inv_a, (0.5 * LOG2E) * inv_c, LOG2E * cross
    xs = [(4 * (row8 % 4) + r).astype(F32) + 0.5 for r in range(NPX)]
    ys = (2 * iota((8, 8, GP), 0) + iota((8, 8, GP), 1) // 4).astype(F32) + 0.5

    lane256 = iota((256, GP), 1)
    total = jnp.zeros((256, 64), F32)
    logs = jnp.zeros((256, GP), F32)
    for b in range(BLK):
        of = lambda v: jnp.broadcast_to(v[b : b + 1, :], (8, GP))
        mx, my, ca, cc, cb, op = (of(v) for v in (mean_x, mean_y, half_a, half_c, cross2, log_op))
        dy = ys - my[None]
        part_y = op[None] - cc[None] * dy * dy
        slope = cb[None] * dy
        covs = []
        for r in range(NPX):
            dx = xs[r] - mx
            covs.append(jnp.exp2(part_y - (ca * dx * dx)[None] - dx[None] * slope))
        cov = jnp.stack(covs, axis=0).reshape(256, GP)
        before = mm(jnp.concatenate(split(jnp.log(1.0 - cov)), axis=1), before_of)
        weight = jnp.exp(before[:, 0:GP]) * cov
        logs = jnp.where(lane256 == 4 * b + 3, before[:, GP:], logs)
        c_hi, c_lo = split(jnp.where(row32 // 4 == b, crow, 0.0))
        both = jnp.concatenate(
            [jnp.concatenate([c_hi, c_hi], axis=1), jnp.concatenate([c_lo, jnp.zeros((32, GP), BF16)], axis=1)], axis=0
        )
        total += mm_nt(jnp.concatenate(split(weight), axis=1), both)
        w_ref[b] = weight
        u_ref[b] = cov
    total = jnp.concatenate([total, jnp.zeros((256, 64), F32)], axis=1)
    total = jnp.where(lane256 < 32, total + pltpu.roll(total, 96, 1) + logs, 0.0)
    rows = total[0:64]
    for r in range(1, NPX):
        rows += pltpu.roll(total[64 * r : 64 * r + 64], 32 * r, 1)
    rows_ref[...] = rows
    for h in range(HALVES):
        send_b[pl.ds(h, HEADS, stride=4), :] = rows_ref[pl.ds(h, HEADS, stride=2), :]

    pl.semaphore_wait(barrier, jnp.where(head, HEADS - 1 + CELL - 1, HEADS))

    def to_head(pair):
        row = lax.div(pair, 4)
        late = (lax.rem(pair, 4) == 3) & (row >= 3) & (row <= 6)
        peer = jnp.where(late, row + 1, pair + 4 * row)

        @pl.when(peer != own)
        def _():
            pltpu.make_async_remote_copy(
                send_b.at[pl.ds(4 * pair, 3)], recv_b.at[pl.ds(4 * own, 3)], send_sem.at[0], recv_sem.at[0],
                device_id=(cell, peer), device_id_type=MESH,
            ).start()

    def to_two_heads(k, carry):
        to_head(lax.rem(4 * own_y + 16 + k, HEADS))
        to_head(lax.rem(4 * own_y + 47 - k, HEADS))
        return carry

    lax.fori_loop(0, HEADS // 2, to_two_heads, 0)

    for b in range(BLK):
        cov = u_ref[b]
        u_ref[b] = cov / (1.0 - cov)
        wsplit_ref[b] = jnp.concatenate(split(w_ref[b]), axis=1)
        ones_b = jnp.where(row32 == 4 * b + 3, 1.0, 0.0).astype(BF16)
        c_hi, c_lo = split(jnp.where(row32 // 4 == b, crow, 0.0))
        none = jnp.zeros((32, GP), BF16)
        top = jnp.concatenate([c_hi, ones_b], axis=1)
        low = jnp.concatenate([c_lo, none], axis=1)
        wcol_ref[b] = jnp.concatenate([top, low, top, jnp.concatenate([none, none], axis=1)], axis=0)

    def composite():
        for a in range(8):
            lane_in = iota((GP, GP), 0)
            lane_out = iota((GP, GP), 1)
            same = (lane_out // 16 == a) & (lane_out % 4 == lane_in // 32)
            to_own = same & ((lane_out % 16) // 4 == lane_in % 4)
            to_all = same & (lane_in % 4 == 3)
            piece = jnp.concatenate([to_own.astype(F32), to_all.astype(F32)], axis=1).astype(BF16)
            fold_ref[128 * a : 128 * a + 128, :] = piece
            back = (lane_in // 16 == a) & (lane_in % 4 == lane_out // 32) & ((lane_in % 16) // 4 == lane_out % 4)
            back = back.astype(F32).astype(BF16)
            unfold_ref[0:128, 128 * a : 128 * a + 128] = back
            unfold_ref[128:256, 128 * a : 128 * a + 128] = back

        choose_in = iota((GP, 256), 0)
        choose_out = iota((GP, 256), 1)
        choose = (choose_in < 16) & (choose_out < 128) | (choose_in >= 32) & (choose_in < 48) & (choose_out >= 128)
        choose = choose.astype(F32).astype(BF16)
        for i in range(3):
            recv_b[pl.ds(4 * own + i, 1), :] = send_b[pl.ds(4 * pair_of + i, 1), :]
        wait_rows(recv_b, 3 * (OWN - 1), recv_sem.at[0])
        lane8f = lane8.astype(F32)
        block8f = ((lane8 // 4) % 8).astype(F32)
        dense_d = [jnp.zeros((8, GP), F32)] * HALVES
        dense_r = jnp.zeros((8, GP), F32)
        lone = []
        for a in range(8):
            tile_rows = recv_b[pl.ds(32 * a + 2, 8, stride=4), :]
            here = lane8 // 16 == a
            dense_d = [
                jnp.where(here, pltpu.roll(tile_rows, (16 * a - L_DCOL - 16 * h) % GP, 1), dense_d[h]) for h in range(HALVES)
            ]
            dense_r = jnp.where(here, pltpu.roll(tile_rows, (16 * a - L_RANK) % GP, 1), dense_r)
            for entry in range(LIST):
                mine = (lane8 == L_PEER + entry) | (lane8 == L_BLK + entry)
                lone.append(jnp.where(mine, tile_rows, 0.0))
        named = mm(jnp.concatenate(lone, axis=0).astype(BF16), choose).reshape(96, 8, 256)
        hot = jnp.where(named[:, :, 0:128] == lane8f[None], 1.0, 0.0).reshape(768, GP)
        pick = jnp.where(named[:, :, 128:256] == block8f[None], 1.0, 0.0).reshape(768, GP).astype(BF16)
        hot_ref[...] = hot
        pick_ref[...] = pick
        dense_d = [jnp.where(chan8 < 3, dense_d[h], 0.0) for h in range(HALVES)]

        @pl.when(holder)
        def _():
            for h in range(HALVES):
                send_d[h] = dense_d[h]
                recv_d[h] = dense_d[h]
            for i in CELL_ORDER:
                pltpu.make_async_remote_copy(
                    send_d, recv_d, send_sem.at[2], recv_sem.at[2],
                    device_id=(lax.rem(cell + i, CELL), own), device_id_type=MESH,
                ).start()

        one_rank = jnp.concatenate([jnp.where(lane8 % 16 == c, dense_r, 0.0) for c in range(CELL)], axis=0)
        group = (iota((GP, GP), 0) // 16 == iota((GP, GP), 1) // 16).astype(F32).astype(BF16)
        rank_ref[...] = mm(one_rank.astype(BF16), group).reshape(8, 8, GP)

        pieces = []
        for h in range(HALVES):
            pieces += split(recv_b[pl.ds(h, 64, stride=4), :])
        taken = mm(hot.astype(BF16)[:, 0:64], jnp.concatenate(pieces, axis=1)).astype(BF16)
        taken = taken * jnp.concatenate([pick] * 4, axis=1)
        taken = jnp.concatenate(
            [
                jnp.concatenate([taken[96 * a : 96 * a + 96, 128 * g : 128 * g + 128] for a in range(8)], axis=1)
                for g in range(2 * HALVES)
            ],
            axis=0,
        )
        folded = mm(taken, fold_ref[...]).reshape(HALVES, 2, 96, 256)
        folded = (folded[:, 0] + folded[:, 1]).reshape(HALVES * 96, 256)
        entry_c = folded[:, 0:128].reshape(HALVES, LIST, 8, GP)
        entry_t = folded[:, 128:256].reshape(HALVES, LIST, 8, GP)
        for h in range(HALVES):
            ahead = jnp.zeros((8, GP), F32)
            part = jnp.zeros((8, GP), F32)
            for entry in range(LIST):
                seen = jnp.exp(ahead)
                dens_ref[h, entry] = seen
                part += seen * entry_c[h, entry]
                ahead += entry_t[h, entry]
            all_x[cell, h] = jnp.where(chan8 < 3, part, ahead)
        for i in CELL_ORDER:
            pltpu.make_async_remote_copy(
                all_x.at[cell], all_x.at[cell], send_sem.at[3], recv_sem.at[3],
                device_id=(lax.rem(cell + i, CELL), own), device_id_type=MESH,
            ).start()

        hot_t_ref[...] = hot_ref[...].T[0:64].astype(BF16)
        ranks = [rank_ref[c] for c in range(CELL)]

        @pl.when(jnp.logical_not(holder))
        def _():
            pltpu.make_async_copy(recv_d, recv_d, recv_sem.at[2]).wait()

        wait_rows(all_x, CELL - 1, recv_sem.at[3])

        grad_rows = []
        colours = []
        my_rank = rank_ref[cell]
        for h in range(HALVES):
            dense = recv_d[h]
            parts = [all_x[c, h] for c in range(CELL)]
            logs, dots = [], []
            for c in range(CELL):
                last = jnp.where(chan8 == 3, parts[c], 0.0)
                logs.append(last + pltpu.roll(last, 124, 1) + pltpu.roll(last, 120, 1) + pltpu.roll(last, 116, 1))
                lossy = parts[c] * dense
                dots.append(pltpu.roll(lossy, 4, 1) + pltpu.roll(lossy, 8, 1) + pltpu.roll(lossy, 12, 1))
            colour = jnp.zeros((8, GP), F32)
            behind = jnp.zeros((8, GP), F32)
            for c in range(CELL):
                shade = jnp.zeros((8, GP), F32)
                for other in range(CELL):
                    if other != c:
                        shade += jnp.where(ranks[other] < ranks[c], logs[other], 0.0)
                lit = jnp.exp(shade)
                lit_ref[h, c] = lit
                colour += lit * parts[c]
                behind += jnp.where(ranks[c] > my_rank, lit * dots[c], 0.0)
            colours.append(colour)
            d_part = dense * lit_ref[h, cell]
            of_half = [None] * LIST
            for entry in reversed(range(LIST)):
                d_c = dens_ref[h, entry] * d_part
                of_half[entry] = jnp.where(chan8 < 3, d_c, behind)
                lossy = d_c * entry_c[h, entry]
                behind = behind + (pltpu.roll(lossy, 4, 1) + pltpu.roll(lossy, 8, 1) + pltpu.roll(lossy, 12, 1))
            grad_rows += of_half
        pick = pick_ref[...]
        g_hi, g_lo = split(jnp.concatenate(grad_rows, axis=0))
        wide = mm(jnp.concatenate([g_hi, g_lo], axis=1), unfold_ref[...])
        columns = []
        for h in range(HALVES):
            spread = jnp.concatenate([wide[96 * h : 96 * h + 96, 128 * a : 128 * a + 128] for a in range(8)], axis=0)
            spread_hi, spread_lo = split(spread)
            columns += [spread_hi * pick, spread_lo * pick]
        back = mm(hot_t_ref[...], jnp.concatenate(columns, axis=1))
        for h in range(HALVES):
            send_f[pl.ds(h, 64, stride=2), :] = back[:, 256 * h : 256 * h + 128] + back[:, 256 * h + 128 : 256 * h + 256]
        early_first(
            lambda peer: pltpu.make_async_remote_copy(
                send_f.at[pl.ds(2 * peer, 2)], recv_f.at[pl.ds(2 * pair_of, 2)], send_sem.at[4], recv_sem.at[4],
                device_id=(cell, peer), device_id_type=MESH,
            ).start()
        )
        for i in range(HALVES):
            recv_f[pl.ds(2 * pair_of + i, 1), :] = send_f[pl.ds(2 * own + i, 1), :]

        @pl.when(holder)
        def _():
            for h in range(HALVES):
                for a in range(8):
                    send_c[pl.ds(16 * a + h, 8, stride=2), :] = pltpu.roll(colours[h], (GP - 16 * a) % GP, 1)
            early_first(
                lambda peer: pltpu.make_async_remote_copy(
                    send_c.at[pl.ds(2 * peer, 2)], recv_c.at[pl.ds(2 * pair_z, 2)], send_sem.at[5], recv_sem.at[5],
                    device_id=(cell, peer), device_id_type=MESH,
                ).start()
            )
            for i in range(HALVES):
                recv_c[pl.ds(2 * pair_z + i, 1), :] = send_c[pl.ds(2 * own + i, 1), :]

    @pl.when(head)
    def _():
        composite()

    after_of = (iota((2 * GP, GP), 0) % GP > iota((2 * GP, GP), 1)).astype(F32).astype(BF16)

    @pl.when(head)
    def _():
        wait_rows(recv_f, OWN - 2, recv_sem.at[4])

    @pl.when(not_head)
    def _():
        wait_rows(recv_f, OWN, recv_sem.at[4])

    cot = recv_f[...]
    cot_hi = cot.astype(BF16).astype(F32)
    cot_lo = cot - cot_hi
    lane64 = iota((64, GP), 1)
    left = []
    for r in range(NPX):
        one = pltpu.roll(cot_hi, (GP - 32 * r) % GP, 1)
        two = pltpu.roll(cot_hi, (GP + 32 - 32 * r) % GP, 1)
        three = pltpu.roll(cot_lo, (GP + 64 - 32 * r) % GP, 1)
        left.append(jnp.where(lane64 < 32, one, jnp.where(lane64 < 64, two, jnp.where(lane64 < 96, three, 0.0))))
    left = jnp.concatenate(left, axis=0).astype(BF16)
    turned = jnp.concatenate([cot, jnp.zeros((64, GP), F32)], axis=0).T
    turned = jnp.concatenate(
        [
            turned[0:32] + pltpu.roll(turned[32:64], 64, 1),
            turned[64:96] + pltpu.roll(turned[96:128], 64, 1),
        ],
        axis=1,
    )
    turned = jnp.concatenate(split(turned), axis=0)
    d_colour = jnp.zeros((32, GP), F32)
    for b in range(BLK):
        of = lambda v: jnp.broadcast_to(v[b : b + 1, :], (8, GP))
        mx, my = of(mean_x), of(mean_y)
        pair = mm(left, wcol_ref[b])
        d_before = pair[:, 0:128] * w_ref[b]
        after = mm(jnp.concatenate(split(d_before), axis=1), after_of)
        flow = (d_before - (pair[:, 128:256] + after) * u_ref[b]).reshape(NPX, 8, 8, GP)
        dy = ys - my[None]
        m0 = mxs = mxx = mys = mxy = myy = jnp.zeros((8, GP), F32)
        for r in range(NPX):
            dx = xs[r] - mx
            q = flow[r]
            qy = q * dy
            s0, s1 = jnp.sum(q, axis=0), jnp.sum(qy, axis=0)
            m0 += s0
            mxs += s0 * dx
            mxx += s0 * dx * dx
            mys += s1
            mxy += s1 * dx
            myy += jnp.sum(qy * dy, axis=0)
        for i, m in enumerate((m0, mxs, mxx, mys, mxy, myy)):
            mom_ref[i, b : b + 1, :] = jnp.sum(m, axis=0, keepdims=True)
    for b in range(BLK):
        grown = mm(turned, wsplit_ref[b])
        grown = grown[0:32, 0:128] + grown[0:32, 128:256] + grown[32:64, 0:128]
        d_colour = jnp.where(row32 // 4 == b, grown, d_colour)
    m0, mxs, mxx, mys, mxy, myy = (mom_ref[i] for i in range(6))
    grad_ref[0] = inv_a * mxs + cross * mys
    grad_ref[1] = inv_c * mys + cross * mxs
    grad_ref[2] = -0.5 * (inv_a * mxx + cross * mxy)
    grad_ref[3] = -0.5 * (inv_c * myy + cross * mxy)
    grad_ref[4] = -mid * mxy
    grad_ref[5] = (1.0 - opacity) * m0
    crow_ref[...] = d_colour
    for k in range(3):
        grad_ref[6 + k] = crow_ref[pl.ds(k, 8, stride=4), :]

    @pl.when(holder)
    def _():
        wait_rows(recv_c, 6, recv_sem.at[5])

    @pl.when(jnp.logical_not(holder))
    def _():
        wait_rows(recv_c, 8, recv_sem.at[5])

    tile = pltpu.roll(recv_c[...], 0, 1, stride=4, stride_axis=0)
    for k in range(3):
        moved = pltpu.roll(tile, (GP - 4 * k) % GP, 1)
        moved = jnp.where(lane8 // 4 == row8, moved, 0.0)
        colour_ref[k] = jnp.sum(moved, axis=0, keepdims=True)[:, 0:32]

    @pl.when(head)
    def _():
        wait_rows(send_b, 3 * (HEADS - 1), send_sem.at[0])
        wait_rows(send_f, 2 * (OWN - 1), send_sem.at[4])
        wait_rows(all_x, CELL - 1, send_sem.at[3])

    @pl.when(not_head)
    def _():
        wait_rows(send_b, 3 * HEADS, send_sem.at[0])

    @pl.when(holder)
    def _():
        wait_rows(send_c, 2 * (OWN - 1), send_sem.at[5])
        wait_rows(all_x, CELL - 1, send_sem.at[2])


def put(colour_ref, grad_ref, colour_out, grad_out, sem):
    one = pltpu.make_async_copy(colour_ref, colour_out, sem.at[0])
    two = pltpu.make_async_copy(grad_ref, grad_out, sem.at[1])
    two.start()
    one.start()
    two.wait()
    one.wait()


def finish(colour, grads):
    vmem = pl.BlockSpec(memory_space=pltpu.VMEM)
    hbm = pl.BlockSpec(memory_space=pltpu.HBM)
    return pl.pallas_call(
        put,
        out_shape=(jax.ShapeDtypeStruct(colour.shape, F32), jax.ShapeDtypeStruct(grads.shape, F32)),
        in_specs=[vmem, vmem],
        out_specs=(hbm, hbm),
        scratch_shapes=[pltpu.SemaphoreType.DMA((2,))],
        compiler_params=pltpu.CompilerParams(vmem_limit_bytes=1 << 20),
    )(colour, grads)


def body(gaussians, fetch_ids, tile_lists, counts, cell_rank, d_colour):
    fetch = jnp.transpose(fetch_ids, (0, 1, 3, 2)).reshape(CAP, OWN)
    lists = tile_lists.reshape(1, LIST)
    hb = lambda v: pltpu.with_memory_space_constraint(v, pltpu.HBM)
    params = jnp.transpose(gaussians, (1, 0, 2))
    d_rows = jnp.transpose(d_colour, (1, 0, 2))
    hbm = pl.BlockSpec(memory_space=pltpu.HBM)
    vmem = pl.BlockSpec(memory_space=pltpu.VMEM)
    row = lambda n: pltpu.VMEM((n, GP), F32)
    colour, grads = pl.pallas_call(
        kernel,
        out_shape=(
            jax.ShapeDtypeStruct((3, 1, 32), F32),
            jax.ShapeDtypeStruct((9, BLK, GP), F32),
        ),
        in_specs=[hbm] * 6,
        out_specs=(vmem, vmem),
        scratch_shapes=[
            pltpu.SMEM((CAP, OWN), jnp.int32),
            pltpu.SMEM((1, LIST), jnp.int32),
            pltpu.SMEM((1, 1), jnp.int32),
            pltpu.SMEM((1, CELL), jnp.int32),
            pltpu.VMEM((9, BLK, GP), F32),
            pltpu.VMEM((3, 1, 32), F32),
            pltpu.SemaphoreType.DMA((6,)),
            pltpu.VMEM((BLK, 256, GP), F32),
            pltpu.VMEM((BLK, 256, GP), F32),
            pltpu.VMEM((BLK, 256, 256), BF16),
            pltpu.VMEM((BLK, GP, 256), BF16),
            pltpu.VMEM((32, GP), F32),
            pltpu.VMEM((6, 8, GP), F32),
            pltpu.VMEM((8, GP), F32),
            pltpu.VMEM((64, GP), F32),
            pltpu.VMEM((1024, 256), BF16),
            pltpu.VMEM((256, 1024), BF16),
            pltpu.VMEM((768, GP), F32),
            pltpu.VMEM((768, GP), BF16),
            pltpu.VMEM((64, 768), BF16),
            pltpu.VMEM((8, 8, GP), F32),
            pltpu.VMEM((HALVES, 8, 8, GP), F32),
            pltpu.VMEM((HALVES, LIST, 8, GP), F32),
            row(128), row(256),
            pltpu.VMEM((8, HALVES, 8, GP), F32),
            pltpu.VMEM((HALVES, 8, GP), F32),
            pltpu.VMEM((HALVES, 8, GP), F32),
            row(128), row(64), row(128), row(8),
            pltpu.SemaphoreType.DMA((6,)),
            pltpu.SemaphoreType.DMA((6,)),
        ],
        compiler_params=pltpu.CompilerParams(
            collective_id=0, has_side_effects=True, vmem_limit_bytes=32 << 20
        ),
    )(hb(fetch), hb(lists), counts, hb(cell_rank), hb(params), hb(d_rows))
    colour, grads = finish(colour, grads)
    return jnp.transpose(colour, (1, 0, 2)), jnp.transpose(grads, (1, 0, 2))


def solution(mesh):
    in_specs = (
        P(("cell", "own"), None, None),
        P("cell", "own", None, None),
        P("cell", "own", None),
        P("cell", "own"),
        P("own", None),
        P("own", None, "cell"),
    )
    out_specs = (P("own", None, "cell"), P(("cell", "own"), None, None))
    return jax.shard_map(body, mesh=mesh, in_specs=in_specs, out_specs=out_specs, check_vma=False)
```
